128 devices in a mesh: seq: 64 (over z, x, y), batch: 2 (over core).
Axes of the slice: x: 4, y: 4, z: 4, core: 2. Of those that a mesh axis runs over, the one named last changes fastest.
Arguments:
- inputs: bfloat16 [2, 8192, 2048], P('batch', 'seq'), may hold values from -6 to 6
- cotangent: bfloat16 [2, 8192, 1024], P('batch', 'seq'), may hold values from -48 to 48
- w_query: bfloat16 [2048, 128], replicated, may hold values from -0.125 to 0.125
- w_key: bfloat16 [2048, 128], replicated, may hold values from -0.125 to 0.125
- w_value: bfloat16 [2048, 1024], replicated, may hold values from -0.125 to 0.125
Outputs:
- grad_inputs: bfloat16 [2, 8192, 2048], P('batch', 'seq')
- grad_w_query: float32 [2048, 128], P(('seq', 'batch'))
- grad_w_key: float32 [2048, 128], P(('seq', 'batch'))
- grad_w_value: float32 [2048, 1024], P(('seq', 'batch'))
The draws below stay inside these ranges and needn't reach their ends.
All inputs are finite; a program needn't handle non-finite values.
Results may differ from the reference program's by a relative error of at most 0.006.
Values sent between devices are 32-bit elements; how exact they have to be, the bound alone decides.
A program may use at most 128 MiB of HBM per device.

```python
import math
import jax
import jax.numpy as jnp
import numpy as np
from jax import lax

D = 2048
H = 8
DK = 16
DV = 128
F = 153
SEQ_LEN = 8192
SEQS = 2


def shard_levels(stream_key, shape, cuts, least, high):
    gain, own = 1.0, jax.random.fold_in(stream_key, 6)
    for position, parts in cuts:
        draws = jnp.exp(jax.random.uniform(jax.random.fold_in(own, position), (parts,), jnp.float32, least / len(cuts), high / len(cuts)))
        gain = gain * jnp.repeat(draws, shape[position] // parts).reshape([-1 if axis == position else 1 for axis in range(len(shape))])
    return gain


def bell_draw(stream_key, extent, scale, bound, cuts=(), kind=jnp.bfloat16):
    drawn = scale * jax.random.normal(stream_key, extent, jnp.float32)
    if cuts:
        drawn = drawn * shard_levels(stream_key, extent, cuts, -0.22, 0.18)
    return jnp.clip(drawn, -bound, bound).astype(kind)


def setup_inputs(seed: int = 0) -> dict:
    streams_of = jax.random.split(jax.random.key(seed), 6)
    inputs = bell_draw(streams_of[0], (SEQS, SEQ_LEN, D), 1.0, 6.0, ((0, 2), (1, 64)))
    cotangent = bell_draw(streams_of[1], (SEQS, SEQ_LEN, H * DV), 8.0, 48.0, ((0, 2), (1, 64)))
    w_query = bell_draw(streams_of[2], (D, H * DK), D ** -0.5, 0.125)
    w_key = bell_draw(streams_of[3], (D, H * DK), D ** -0.5, 0.125)
    w_value = bell_draw(streams_of[4], (D, H * DV), D ** -0.5, 0.125)
    return dict(inputs=inputs, cotangent=cotangent, w_query=w_query, w_key=w_key, w_value=w_value)


highest = lax.Precision.HIGHEST

def pair_tables(width):
    rows_idx, cols_idx = np.triu_indices(width)
    eye_table = np.eye(width, dtype=np.float32)
    left_pick = jnp.asarray(eye_table[rows_idx])
    right_pick = jnp.asarray(eye_table[cols_idx])
    pair_coef = jnp.asarray(np.where(rows_idx == cols_idx, 1.0 / math.sqrt(2.0), 1.0).astype(np.float32))
    return (left_pick, right_pick, pair_coef)

def features(scaled, tables):
    left_pick, right_pick, pair_coef = tables
    left_val = jnp.einsum('...d,pd->...p', scaled, left_pick, precision=highest)
    right_val = jnp.einsum('...d,pd->...p', scaled, right_pick, precision=highest)
    leading = jnp.ones(scaled.shape[:-1] + (1,), jnp.float32)
    return jnp.concatenate([leading, scaled, left_val * right_val * pair_coef], -1)

def pull_back(scaled, grad_feat, tables):
    left_pick, right_pick, pair_coef = tables
    width = scaled.shape[-1]
    linear_part = grad_feat[..., 1:1 + width]
    pair_grad = grad_feat[..., 1 + width:] * pair_coef
    left_val = jnp.einsum('...d,pd->...p', scaled, left_pick, precision=highest)
    right_val = jnp.einsum('...d,pd->...p', scaled, right_pick, precision=highest)
    result = linear_part + jnp.einsum('...p,pd->...d', pair_grad * right_val, left_pick, precision=highest)
    return result + jnp.einsum('...p,pd->...d', pair_grad * left_val, right_pick, precision=highest)

def reference(inputs, cotangent, w_query, w_key, w_value):
    tables = pair_tables(DK)
    flat = inputs.reshape(SEQS * SEQ_LEN, D)
    query = jnp.dot(flat, w_query, preferred_element_type=jnp.float32).reshape(SEQS, SEQ_LEN, H, DK)
    keys = jnp.dot(flat, w_key, preferred_element_type=jnp.float32).reshape(SEQS, SEQ_LEN, H, DK)
    values = jnp.dot(flat, w_value, preferred_element_type=jnp.float32).astype(jnp.bfloat16).reshape(SEQS, SEQ_LEN, H, DV)
    feat_q = features(query * 0.5, tables).astype(jnp.bfloat16)
    feat_k = features(keys * 0.5, tables).astype(jnp.bfloat16)
    upstream = cotangent.astype(jnp.float32).reshape(SEQS, SEQ_LEN, H, DV)
    block_len = math.gcd(512, SEQ_LEN)
    nblocks = SEQ_LEN // block_len

    def blocked(array):
        return array.reshape((SEQS, nblocks, block_len) + array.shape[2:]).swapaxes(0, 1)

    def unblocked(array):
        return array.swapaxes(0, 1).reshape((SEQS, SEQ_LEN) + array.shape[3:])
    causal = lax.broadcasted_iota(jnp.int32, (block_len, block_len), 0) >= lax.broadcasted_iota(jnp.int32, (block_len, block_len), 1)

    def scores(fq32, fk32):
        attn = jnp.einsum('bthf,bshf->bhts', fq32, fk32, precision=highest)
        return jnp.where(causal, attn, 0.0)

    def grad_scores(grad_numer, grad_denom, val32):
        inner = jnp.einsum('bthe,bshe->bhts', grad_numer, val32, precision=highest)
        inner = inner + jnp.transpose(grad_denom, (0, 2, 1))[:, :, :, None]
        return jnp.where(causal, inner, 0.0)

    def forward_step(carry, pieces):
        state, norm_state = carry
        fq_blk, fk_blk, val_blk, up_blk = pieces
        fq32 = fq_blk.astype(jnp.float32)
        fk32 = fk_blk.astype(jnp.float32)
        val32 = val_blk.astype(jnp.float32)
        attn = scores(fq32, fk32)
        numerator = jnp.einsum('bhts,bshe->bthe', attn, val32, precision=highest)
        numerator = numerator + jnp.einsum('bthf,bhfe->bthe', fq32, state, precision=highest)
        denominator = jnp.transpose(lax.optimization_barrier(jnp.sum(attn, -1)), (0, 2, 1))
        denominator = denominator + jnp.einsum('bthf,bhf->bth', fq32, norm_state, precision=highest)
        output = numerator / denominator[..., None]
        grad_numer = up_blk / denominator[..., None]
        grad_denom = -lax.optimization_barrier(jnp.sum(up_blk * output, -1)) / denominator
        grad_attn = grad_scores(grad_numer, grad_denom, val32)
        grad_fq = jnp.einsum('bhts,bshf->bthf', grad_attn, fk32, precision=highest)
        grad_fq = grad_fq + jnp.einsum('bhfe,bthe->bthf', state, grad_numer, precision=highest)
        grad_fq = grad_fq + norm_state[:, None, :, :] * grad_denom[..., None]
        state = state + jnp.einsum('bshf,bshe->bhfe', fk32, val32, precision=highest)
        norm_state = norm_state + lax.optimization_barrier(jnp.sum(fk32, 1))
        return ((state, norm_state), (grad_numer, grad_denom, grad_fq))
    start_state = (jnp.zeros((SEQS, H, F, DV), jnp.float32), jnp.zeros((SEQS, H, F), jnp.float32))
    _, (grad_numer, grad_denom, grad_fq) = lax.scan(forward_step, start_state, (blocked(feat_q), blocked(feat_k), blocked(values), blocked(upstream)))

    def reverse_step(carry, pieces):
        back_state, back_norm = carry
        fq_blk, fk_blk, val_blk, numer_blk, denom_blk = pieces
        fq32 = fq_blk.astype(jnp.float32)
        fk32 = fk_blk.astype(jnp.float32)
        val32 = val_blk.astype(jnp.float32)
        attn = scores(fq32, fk32)
        grad_attn = grad_scores(numer_blk, denom_blk, val32)
        grad_val = jnp.einsum('bhts,bthe->bshe', attn, numer_blk, precision=highest)
        grad_val = grad_val + jnp.einsum('bshf,bhfe->bshe', fk32, back_state, precision=highest)
        grad_fk = jnp.einsum('bhts,bthf->bshf', grad_attn, fq32, precision=highest)
        grad_fk = grad_fk + jnp.einsum('bshe,bhfe->bshf', val32, back_state, precision=highest)
        grad_fk = grad_fk + back_norm[:, None, :, :]
        back_state = back_state + jnp.einsum('bthf,bthe->bhfe', fq32, numer_blk, precision=highest)
        back_norm = back_norm + jnp.einsum('bthf,bth->bhf', fq32, denom_blk, precision=highest)
        return ((back_state, back_norm), (grad_val, grad_fk))
    _, (grad_val, grad_fk) = lax.scan(reverse_step, start_state, (blocked(feat_q), blocked(feat_k), blocked(values), grad_numer, grad_denom), reverse=True)
    grad_fq = unblocked(grad_fq)
    grad_fk = unblocked(grad_fk)
    grad_val = unblocked(grad_val)
    grad_query = (pull_back(query * 0.5, grad_fq, tables) * 0.5).astype(jnp.bfloat16).reshape(SEQS * SEQ_LEN, H * DK)
    grad_keys = (pull_back(keys * 0.5, grad_fk, tables) * 0.5).astype(jnp.bfloat16).reshape(SEQS * SEQ_LEN, H * DK)
    grad_values = grad_val.astype(jnp.bfloat16).reshape(SEQS * SEQ_LEN, H * DV)
    grad_in = jnp.dot(grad_query, w_query.T, preferred_element_type=jnp.float32)
    grad_in = grad_in + jnp.dot(grad_keys, w_key.T, preferred_element_type=jnp.float32)
    grad_in = grad_in + jnp.dot(grad_values, w_value.T, preferred_element_type=jnp.float32)
    grad_in = grad_in.astype(jnp.bfloat16).reshape(SEQS, SEQ_LEN, D)
    grad_wq = jnp.dot(flat.T, grad_query, preferred_element_type=jnp.float32)
    grad_wk = jnp.dot(flat.T, grad_keys, preferred_element_type=jnp.float32)
    grad_wv = jnp.dot(flat.T, grad_values, preferred_element_type=jnp.float32)
    return (grad_in, grad_wq, grad_wk, grad_wv)
```

```python
import math

import jax
import jax.numpy as jnp
from jax import lax
from jax.experimental import pallas as pl
from jax.experimental.pallas import tpu as pltpu
from jax.sharding import Mesh
from jax.sharding import PartitionSpec as P

D = 2048
H = 8
DK = 16
DV = 128
SEQ = ("seq_0", "seq_1", "seq_2")
SEQ_BATCH = ("seq_0", "seq_1", "seq_2", "batch")
N = 4
BLK = 128
TOK = N * BLK
FP = 160
ROOT = 1.0 / math.sqrt(2.0)
ORDER = (1, 3, 2, 0)
f32 = jnp.float32
bf16 = jnp.bfloat16
MESH_ID = pl.DeviceIdType.MESH


def mm(a, b):
    return lax.dot_general(a, b, (((1,), (0,)), ((), ())), preferred_element_type=f32)


def mm_nt(a, b):
    return lax.dot_general(a, b, (((1,), (1,)), ((), ())), preferred_element_type=f32)


def mm_tn(a, b):
    return lax.dot_general(a, b, (((0,), (0,)), ((), ())), preferred_element_type=f32)


def halves(row):
    high = row.astype(bf16).astype(f32)
    return high, row - high


def rows16(*rows):
    n = rows[0].shape[1]
    at = lax.broadcasted_iota(jnp.int32, (16, n), 0)
    out = jnp.zeros((16, n), f32)
    for i, row in enumerate(rows):
        out = jnp.where(at == i, jnp.broadcast_to(row, (16, n)), out)
    return out.astype(bf16)


def turned(u, d):
    d = d % DK
    return u if d == 0 else pltpu.roll(u, DK - d, 0)


def features(u):
    n = u.shape[1]
    parts = [u, u * u * ROOT]
    for d in range(1, 8):
        parts.append(u * turned(u, d))
    parts.append(u[:8] * u[8:])
    first = lax.broadcasted_iota(jnp.int32, (8, n), 0) == 0
    parts.append(jnp.where(first, 1.0, 0.0).astype(f32))
    return jnp.concatenate(parts, 0).astype(bf16)


def pull_back(u, g):
    out = g[0:16] + (g[16:32] * (2.0 * ROOT)) * u
    for d in range(1, 8):
        pair = g[16 + 16 * d : 32 + 16 * d]
        out = out + pair * turned(u, d) + turned(pair * u, -d)
    pair = g[144:152]
    return out + jnp.concatenate([pair * u[8:], pair * u[:8]], 0)


def kernel(
    x_hbm, u_hbm, wq_hbm, wk_hbm, wv_hbm,
    gin, gwq, gwk, gwv,
    xb, ub, wq, wk, wv, xt2, xg,
    sqk, sv, rqk, rv, us, ur,
    fq, fk, vb, vt, ut, at, num, dloc, gnb, gdr, gfq, gfk, gvt, stb, nrm,
    st1, xr1, zs1, zr1, pb1, pf1,
    st2, xr2, zs2, zr2, pb2, pf2,
    gg, gb, d1, d2, r1, r2, s1, s2, t1, t2, yb, yr,
    lsem, ssem, rsem,
):
    z, x, y, c = (lax.axis_index(a) for a in SEQ_BATCH)
    place = {"seq_0": z, "seq_1": x, "seq_2": y}
    started = []
    used = [0]

    def send(src, dst, target):
        k = used[0]
        used[0] += 1
        copy = pltpu.make_async_remote_copy(
            src_ref=src, dst_ref=dst, send_sem=ssem.at[k], recv_sem=rsem.at[k],
            device_id=target, device_id_type=MESH_ID,
        )
        copy.start()
        started.append(copy)
        return copy

    def at_peer(axis, d):
        return lax.rem(place[axis] + d, N)

    loads = {}

    def load(name, k, src, dst):
        loads[name] = pltpu.make_async_copy(src, dst, lsem.at[k])
        loads[name].start()

    load("x", 0, x_hbm.at[0], xb)
    load("wq", 1, wq_hbm, wq)
    load("wk", 2, wk_hbm, wk)
    for k, dy in enumerate(ORDER):
        cols = pl.ds(pl.multiple_of(at_peer("seq_2", dy) * 256, 256), 256)
        load(("wv", k), 3 + k, wv_hbm.at[:, cols], wv.at[k])
    load("u", 7, u_hbm.at[0], ub)

    barrier = pltpu.get_barrier_semaphore()
    for axis in SEQ:
        for d in (1, 2, 3):
            pl.semaphore_signal(
                barrier, inc=1, device_id={axis: at_peer(axis, d)}, device_id_type=MESH_ID
            )
    pl.semaphore_signal(barrier, inc=1, device_id={"batch": 1 - c}, device_id_type=MESH_ID)

    loads["x"].wait()
    loads["wq"].wait()
    qt = mm(xb[...], wq[...]).T
    loads["wk"].wait()
    kt = mm(xb[...], wk[...]).T
    for p in range(N):
        sqk[p, 0:32] = qt[32 * p : 32 * p + 32]
        sqk[p, 32:64] = kt[32 * p : 32 * p + 32]
    pl.semaphore_wait(barrier, 10)
    qk_in = []
    for dy in (1, 3, 2):
        p = at_peer("seq_2", dy)
        qk_in.append(send(sqk.at[p], rqk.at[y], {"seq_2": p}))
    rqk[y] = sqk[y]
    v_in = []
    for k, dy in enumerate(ORDER):
        p = at_peer("seq_2", dy)
        loads[("wv", k)].wait()
        v = mm(xb[...], wv[k]).astype(bf16).astype(f32)
        if dy:
            sv[k] = v
            v_in.append(send(sv.at[k], rv.at[y], {"seq_2": p}))
        else:
            rv[y] = v
    loads["u"].wait()
    for p in range(N):
        us[p] = ub[:, 256 * p : 256 * p + 256].astype(f32)
    u_in = []
    for dy in (1, 3, 2):
        p = at_peer("seq_2", dy)
        u_in.append(send(us.at[p], ur.at[y], {"seq_2": p}))
    ur[y] = us[y]

    for b in range(16):
        block = xb[:, 128 * b : 128 * b + 128].astype(f32).T
        for i in range(8):
            row = 64 * b + 16 * (i // 2)
            xt2[i % 2, row : row + 16] = block[16 * i : 16 * i + 16]
    pair_x = send(xt2.at[1 - c], xg.at[y, c], {"batch": 1 - c})
    xg[y, c] = xt2[c]

    for copy in qk_in:
        copy.wait_recv()
    us_q, us_k = [], []
    for h in range(2):
        lo = 16 * h
        uq = jnp.concatenate([rqk[j, lo : lo + 16] for j in range(N)], 1) * 0.5
        uk = jnp.concatenate([rqk[j, 32 + lo : 48 + lo] for j in range(N)], 1) * 0.5
        fq[h] = features(uq)
        fk[h] = features(uk)
    for copy in v_in:
        copy.wait_recv()
    ones = jnp.ones((16, TOK), bf16)
    for h in range(2):
        for j in range(N):
            vb[h, 128 * j : 128 * j + 128] = rv[j, :, 128 * h : 128 * h + 128].astype(bf16)

    def put_state(st, h, state, norm):
        st[2 * h] = state[:80]
        st[2 * h + 1] = state[80:]
        st[2 * h + 1, 73:74] = norm[:, :128]
        st[2 * h + 1, 74:75] = jnp.concatenate([norm[:, 128:], jnp.zeros((1, 96), f32)], 1)

    def get_state(pf, h):
        state = jnp.concatenate([pf[2 * h], pf[2 * h + 1]], 0)
        norm = jnp.concatenate([pf[2 * h + 1, 73:74], pf[2 * h + 1, 74:75, :32]], 1)
        return state, norm

    for h in range(2):
        put_state(st1, h, mm(fk[h], vb[h]), mm_nt(ones, fk[h])[:1])

    def scan_start(st, xr):
        copies = []
        for d in (1, 3, 2):
            p = at_peer("seq_1", d)
            copies.append(send(st.at[p], xr.at[x], {"seq_1": p}))
        xr[x] = st[x]
        return copies

    def scan_mid(copies, xr, zs, zr):
        for copy in copies:
            copy.wait_recv()
        zs[...] = (xr[0] + xr[1]) + (xr[2] + xr[3])
        return [send(zs, zr.at[z], {"seq_0": at_peer("seq_0", d)}) for d in (1, 3, 2)]

    def scan_back(copies, xr, zr, pb, pf, later):
        for copy in copies:
            copy.wait_recv()
        run = jnp.zeros((80, 128), f32)
        for d in (1, 2, 3):
            p = at_peer("seq_0", d)
            run = run + jnp.where(p > z if later else p < z, zr[p], 0.0)
        for i in reversed(range(N)) if later else range(N):
            pb[i] = run
            run = run + xr[i]
        out = []
        for d in (1, 3, 2):
            p = at_peer("seq_1", d)
            out.append(send(pb.at[p], pf.at[x], {"seq_1": p}))
        pf[x] = pb[x]
        return out

    keep = lax.broadcasted_iota(jnp.int32, (TOK, TOK), 1) >= lax.broadcasted_iota(
        jnp.int32, (TOK, TOK), 0
    )

    def local_forward(h):
        for j in range(N):
            vt[h, :, 128 * j : 128 * j + 128] = (
                rv[j, :, 128 * h : 128 * h + 128].T.astype(bf16)
            )
        scores = jnp.where(keep, mm_tn(fk[h], fq[h]), 0.0)
        dloc[h] = jnp.broadcast_to(jnp.sum(scores, 0, keepdims=True), (8, TOK))
        at[h] = scores.astype(bf16)
        num[h] = mm(vt[h], at[h])

    move = scan_start(st1, xr1)
    local_forward(0)
    move = scan_mid(move, xr1, zs1, zr1)
    local_forward(1)
    move = scan_back(move, xr1, zr1, pb1, pf1, False)
    pair_x.wait_recv()
    x_in = []
    for dy in (1, 3, 2):
        x_in.append(send(xg.at[y], xg.at[y], {"seq_2": at_peer("seq_2", dy)}))
    for copy in u_in:
        copy.wait_recv()
    for h in range(2):
        for j in range(N):
            ut[h, :, 128 * j : 128 * j + 128] = ur[j, :, 128 * h : 128 * h + 128].T
    for copy in move:
        copy.wait_recv()

    for h in range(2):
        state, norm = get_state(pf1, h)
        stb[h] = state.astype(bf16)
        n_hi, n_lo = halves(norm)
        nrm[h] = jnp.concatenate([n_hi, n_lo, n_hi, jnp.zeros((5, FP), f32)], 0)
        numer = num[h] + mm_tn(stb[h], fq[h])
        denom = dloc[h, :1] + jnp.sum(mm(rows16(n_hi, n_lo), fq[h]), 0, keepdims=True)
        inverse = 1.0 / denom
        upstream = ut[h]
        g_num = upstream * inverse
        g_den = -jnp.sum(upstream * (numer * inverse), 0, keepdims=True) * inverse
        gnb[h] = g_num.astype(bf16)
        g_hi, g_lo = halves(g_den)
        gdr[h] = jnp.concatenate([g_hi, g_lo, jnp.zeros((6, TOK), f32)], 0)
        back = mm_nt(fq[h], gnb[h])
        back_norm = jnp.sum(mm_nt(rows16(g_hi, g_lo), fq[h]), 0, keepdims=True)
        put_state(st2, h, back, back_norm)

    def local_backward(h):
        g_hi, g_lo = gdr[h, 0:1], gdr[h, 1:2]
        n_hi, n_lo = nrm[h, 0:1], nrm[h, 1:2]
        inner = mm(vb[h], gnb[h]) + (g_hi + g_lo)
        ga = jnp.where(keep, inner, 0.0).astype(bf16)
        outer = mm_tn(rows16(n_hi, n_lo, n_hi), rows16(g_hi, g_hi, g_lo))
        gfq[h] = mm(fk[h], ga) + mm(stb[h], gnb[h]) + outer
        gvt[h] = mm_nt(gnb[h], at[h])
        gfk[h] = mm_nt(fq[h], ga)

    def put_grad(h, first, u, grad):
        out = (pull_back(u, grad) * 0.5).astype(bf16).astype(f32)
        for j in range(N):
            gg[c, j, first + 16 * h : first + 16 * h + 16] = out[:, 128 * j : 128 * j + 128]

    move = scan_start(st2, xr2)
    local_backward(0)
    move = scan_mid(move, xr2, zs2, zr2)
    local_backward(1)
    move = scan_back(move, xr2, zr2, pb2, pf2, True)
    for h in range(2):
        lo = 16 * h
        uq = jnp.concatenate([rqk[j, lo : lo + 16] for j in range(N)], 1) * 0.5
        put_grad(h, 256, uq, gfq[h])
    for copy in move:
        copy.wait_recv()
    first16 = lax.broadcasted_iota(jnp.int32, (16, TOK), 0) < 2
    flag = jnp.where(first16, 1.0, 0.0).astype(bf16)
    for h in range(2):
        back, back_norm = get_state(pf2, h)
        backb = back.astype(bf16)
        b_hi, b_lo = halves(back_norm)
        g_val = gvt[h] + mm_tn(backb, fk[h])
        g_val = g_val.astype(bf16).astype(f32)
        for j in range(N):
            gg[c, j, 128 * h : 128 * h + 128] = g_val[:, 128 * j : 128 * j + 128]
        g_fk = gfk[h] + mm(backb, vt[h]) + mm_tn(rows16(b_hi, b_lo), flag)
        lo = 32 + 16 * h
        uk = jnp.concatenate([rqk[j, lo : lo + 16] for j in range(N)], 1) * 0.5
        put_grad(h, 288, uk, g_fk)

    pair_g = send(gg.at[c], gg.at[c], {"batch": 1 - c})
    g_in = []
    for dy in (1, 3, 2):
        p = at_peer("seq_2", dy)
        g_in.append(send(gg.at[c, p], gb.at[y], {"seq_2": p}))
    gb[y] = gg[c, y]

    pair_g.wait_recv()
    for copy in x_in:
        copy.wait_recv()
    rhs = jnp.concatenate([gg[i, j].astype(bf16) for j in range(N) for i in range(2)], 1)

    def weights_of(zz, carry):
        rows = pl.ds(pl.multiple_of(zz * 256, 256), 256)
        lhs = jnp.concatenate([xg[j, i, rows].astype(bf16) for j in range(N) for i in range(2)], 1)
        part = mm_nt(lhs, rhs)
        for xx in range(N):
            own = part[64 * xx : 64 * xx + 64]
            thin = own[:, 256:320]
            thin = jnp.concatenate([thin[:32], thin[32:]], 1)
            d1[xx, zz, 0:64] = own[:, :128]
            d1[xx, zz, 64:80] = own[:16, 128:256]
            d2[zz, xx, 0:48] = own[16:, 128:256]
            d2[zz, xx, 48:80] = thin
        return carry

    lax.fori_loop(0, N, weights_of, 0)

    far1, far2 = [], []
    for i, d in enumerate((1, 3, 2)):
        p = at_peer("seq_1", d)
        far1.append(send(d1.at[p], r1.at[i], {"seq_1": p}))
        p = at_peer("seq_0", d)
        far2.append(send(d2.at[p], r2.at[i], {"seq_0": p}))

    for copy in g_in:
        copy.wait_recv()
    g_q = jnp.concatenate([gb[j, 256:288] for j in range(N)], 0).T.astype(bf16)
    g_k = jnp.concatenate([gb[j, 288:320] for j in range(N)], 0).T.astype(bf16)
    g_v = []
    for k, dy in enumerate(ORDER):
        p = at_peer("seq_2", dy)
        g_v.append(gb[p, 0:256].T.astype(bf16))

    def inputs_of(i, carry):
        rows = pl.ds(pl.multiple_of(i * 512, 512), 512)
        acc = mm_nt(g_q, wq[rows]) + mm_nt(g_k, wk[rows])
        for k in range(N):
            acc = acc + mm_nt(g_v[k], wv[k, rows])
        gin[0, :, rows] = acc.astype(bf16)
        return carry

    lax.fori_loop(0, N, inputs_of, 0)

    for copy in far1:
        copy.wait_recv()
    s1[...] = (d1[x] + r1[0]) + (r1[1] + r1[2])
    near1 = []
    for i, d in enumerate((1, 3, 2)):
        p = at_peer("seq_0", d)
        near1.append(send(s1.at[p], t1.at[i], {"seq_0": p}))
    for copy in far2:
        copy.wait_recv()
    s2[...] = (d2[z] + r2[0]) + (r2[1] + r2[2])
    near2 = []
    for i, d in enumerate((1, 3, 2)):
        p = at_peer("seq_1", d)
        near2.append(send(s2.at[p], t2.at[i], {"seq_1": p}))
    for copy in near1:
        copy.wait_recv()
    one = (s1[z] + t1[0]) + (t1[1] + t1[2])
    for copy in near2:
        copy.wait_recv()
    two = (s2[x] + t2[0]) + (t2[1] + t2[2])
    for j in range(N):
        yb[j, 0:16] = one[16 * j : 16 * j + 16]
        yb[j, 16:32] = one[64:80] if j == 0 else two[16 * j - 16 : 16 * j]
        yb[j, 32:48] = two[48 + 16 * (j % 2) : 64 + 16 * (j % 2)]
    y_in = []
    for dy in (1, 3, 2):
        p = at_peer("seq_2", dy)
        y_in.append(send(yb.at[p], yr.at[y], {"seq_2": p}))
    yr[y] = yb[y]
    for copy in y_in:
        copy.wait_recv()
    lane = lax.broadcasted_iota(jnp.int32, (16, 128), 1) // 32
    w_q = jnp.zeros((16, 128), f32)
    w_k = jnp.zeros((16, 128), f32)
    for p in range(N):
        gwv[:, 256 * p : 256 * p + 128] = yr[p, 0:16]
        gwv[:, 256 * p + 128 : 256 * p + 256] = yr[p, 16:32]
        thin = yr[p, 32:48]
        thin = jnp.where(y >= 2, pltpu.roll(thin, 64, 1), thin)
        from_q = pltpu.roll(thin, 32 * p, 1) if p else thin
        w_q = jnp.where(lane == p, from_q, w_q)
        from_k = pltpu.roll(thin, (32 * p + 96) % 128, 1) if p != 1 else thin
        w_k = jnp.where(lane == p, from_k, w_k)
    gwq[...] = w_q
    gwk[...] = w_k
    for copy in started:
        copy.wait_send()


SENDS = 1 + 3 + 3 + 3 + 3 + 9 + 9 + 1 + 3 + 6 + 6 + 3


def body(inputs, cotangent, w_query, w_key, w_value):
    vmem = pltpu.VMEM
    hbm = pl.BlockSpec(memory_space=pl.ANY)
    here = pl.BlockSpec(memory_space=pltpu.VMEM)
    scan = [
        vmem((4, 80, 128), f32), vmem((4, 80, 128), f32), vmem((80, 128), f32),
        vmem((4, 80, 128), f32), vmem((4, 80, 128), f32), vmem((4, 80, 128), f32),
    ]
    scratch = [
        vmem((BLK, D), bf16), vmem((BLK, 1024), bf16), vmem((D, 128), bf16), vmem((D, 128), bf16),
        vmem((4, D, 256), bf16), vmem((2, 1024, 128), f32), vmem((4, 2, 1024, 128), f32),
        vmem((4, 64, 128), f32), vmem((3, 128, 256), f32), vmem((4, 64, 128), f32),
        vmem((4, 128, 256), f32), vmem((4, 128, 256), f32), vmem((4, 128, 256), f32),
        vmem((2, FP, TOK), bf16), vmem((2, FP, TOK), bf16), vmem((2, TOK, 128), bf16),
        vmem((2, 128, TOK), bf16), vmem((2, 128, TOK), f32), vmem((2, TOK, TOK), bf16),
        vmem((2, 128, TOK), f32), vmem((2, 8, TOK), f32), vmem((2, 128, TOK), bf16),
        vmem((2, 8, TOK), f32), vmem((2, FP, TOK), f32), vmem((2, FP, TOK), f32),
        vmem((2, 128, TOK), f32), vmem((2, FP, 128), bf16), vmem((2, 8, FP), f32),
        *scan, *scan,
        vmem((2, 4, 320, 128), f32), vmem((4, 320, 128), f32),
        vmem((4, 4, 80, 128), f32), vmem((4, 4, 80, 128), f32),
        vmem((3, 4, 80, 128), f32), vmem((3, 4, 80, 128), f32),
        vmem((4, 80, 128), f32), vmem((4, 80, 128), f32),
        vmem((3, 80, 128), f32), vmem((3, 80, 128), f32),
        vmem((4, 48, 128), f32), vmem((4, 48, 128), f32),
        pltpu.SemaphoreType.DMA((8,)), pltpu.SemaphoreType.DMA((SENDS,)),
        pltpu.SemaphoreType.DMA((SENDS,)),
    ]
    return pl.pallas_call(
        kernel,
        out_shape=(
            jax.ShapeDtypeStruct((1, BLK, D), bf16),
            jax.ShapeDtypeStruct((16, 128), f32),
            jax.ShapeDtypeStruct((16, 128), f32),
            jax.ShapeDtypeStruct((16, 1024), f32),
        ),
        in_specs=[hbm] * 5,
        out_specs=(here,) * 4,
        scratch_shapes=scratch,
        compiler_params=pltpu.CompilerParams(
            collective_id=0, has_side_effects=True, vmem_limit_bytes=60 * 1024 * 1024
        ),
    )(inputs, cotangent, w_query, w_key, w_value)


def solution(mesh):
    split = Mesh(
        mesh.devices.reshape(4, 4, 4, mesh.shape["batch"]), ("seq_0", "seq_1", "seq_2", "batch")
    )
    in_specs = (P("batch", SEQ, None), P("batch", SEQ, None), P(), P(), P())
    out_specs = (P("batch", SEQ, None), P(SEQ_BATCH, None), P(SEQ_BATCH, None), P(SEQ_BATCH, None))
    return jax.shard_map(body, mesh=split, in_specs=in_specs, out_specs=out_specs, check_vma=False)
```

```python
import math

import jax
import jax.numpy as jnp
from jax import lax
from jax.experimental import pallas as pl
from jax.experimental.pallas import tpu as pltpu
from jax.sharding import Mesh
from jax.sharding import PartitionSpec as P

D = 2048
H = 8
DK = 16
DV = 128
SEQ = ("seq_0", "seq_1", "seq_2")
SEQ_BATCH = ("seq_0", "seq_1", "seq_2", "batch")
N = 4
BLK = 128
TOK = N * BLK
FP = 160
ROOT = 1.0 / math.sqrt(2.0)
ORDER = (1, 3, 2, 0)
f32 = jnp.float32
bf16 = jnp.bfloat16
MESH_ID = pl.DeviceIdType.MESH


def mm(a, b):
    return lax.dot_general(a, b, (((1,), (0,)), ((), ())), preferred_element_type=f32)


def mm_nt(a, b):
    return lax.dot_general(a, b, (((1,), (1,)), ((), ())), preferred_element_type=f32)


def mm_tn(a, b):
    return lax.dot_general(a, b, (((0,), (0,)), ((), ())), preferred_element_type=f32)


def halves(row):
    high = row.astype(bf16).astype(f32)
    return high, row - high


def rows16(*rows):
    n = rows[0].shape[1]
    at = lax.broadcasted_iota(jnp.int32, (16, n), 0)
    out = jnp.zeros((16, n), f32)
    for i, row in enumerate(rows):
        out = jnp.where(at == i, jnp.broadcast_to(row, (16, n)), out)
    return out.astype(bf16)


def turned(u, d):
    d = d % DK
    return u if d == 0 else pltpu.roll(u, DK - d, 0)


def features(u):
    n = u.shape[1]
    parts = [u, u * u * ROOT]
    for d in range(1, 8):
        parts.append(u * turned(u, d))
    parts.append(u[:8] * u[8:])
    first = lax.broadcasted_iota(jnp.int32, (8, n), 0) == 0
    parts.append(jnp.where(first, 1.0, 0.0).astype(f32))
    return jnp.concatenate(parts, 0).astype(bf16)


def pull_back(u, g):
    out = g[0:16] + (g[16:32] * (2.0 * ROOT)) * u
    for d in range(1, 8):
        pair = g[16 + 16 * d : 32 + 16 * d]
        out = out + pair * turned(u, d) + turned(pair * u, -d)
    pair = g[144:152]
    return out + jnp.concatenate([pair * u[8:], pair * u[:8]], 0)


def kernel(
    x_hbm, u_hbm, wq_hbm, wk_hbm, wv_hbm,
    gin, res,
    xb, ub, wq, wk, wv, xt2, xg,
    sqk, sv, rqk, rv, us, ur,
    fq, fk, vb, vt, ut, at, num, dloc, gnb, gdr, gfq, gfk, gvt, stb, nrm,
    st1, xr1, zs1, zr1, pb1, pf1,
    st2, xr2, zs2, zr2, pb2, pf2,
    gg, gb, gi, da, db, ra, rb, sa, fa, fb,
    lsem, osem, ssem, rsem,
):
    z, x, y, c = (lax.axis_index(a) for a in SEQ_BATCH)
    place = {"seq_0": z, "seq_1": x, "seq_2": y}
    started = []
    used = [0]

    def send(src, dst, target):
        k = used[0]
        used[0] += 1
        copy = pltpu.make_async_remote_copy(
            src_ref=src, dst_ref=dst, send_sem=ssem.at[k], recv_sem=rsem.at[k],
            device_id=target, device_id_type=MESH_ID,
        )
        copy.start()
        started.append(copy)
        return copy

    def at_peer(axis, d):
        return lax.rem(place[axis] + d, N)

    loads = {}

    def load(name, k, src, dst):
        loads[name] = pltpu.make_async_copy(src, dst, lsem.at[k])
        loads[name].start()

    load("x", 0, x_hbm.at[0], xb)
    load("wq", 1, wq_hbm, wq)
    load("wk", 2, wk_hbm, wk)
    for k, dy in enumerate(ORDER):
        cols = pl.ds(pl.multiple_of(at_peer("seq_2", dy) * 256, 256), 256)
        load(("wv", k), 3 + k, wv_hbm.at[:, cols], wv.at[k])
    load("u", 7, u_hbm.at[0], ub)

    barrier = pltpu.get_barrier_semaphore()
    greeted = 0
    for d in range(N):
        for e in range(N):
            pairs = [("seq_0", "seq_2")] if d or e else []
            if d:
                pairs.append(("seq_1", "seq_2"))
            for first, second in pairs:
                greeted += 1
                pl.semaphore_signal(
                    barrier, inc=1, device_id_type=MESH_ID,
                    device_id={first: at_peer(first, d), second: at_peer(second, e)},
                )
        greeted += 1
        pl.semaphore_signal(
            barrier, inc=1, device_id_type=MESH_ID,
            device_id={"seq_2": at_peer("seq_2", d), "batch": 1 - c},
        )

    loads["x"].wait()
    loads["wq"].wait()
    qt = mm(xb[...], wq[...]).T
    loads["wk"].wait()
    kt = mm(xb[...], wk[...]).T
    for p in range(N):
        sqk[p, 0:32] = qt[32 * p : 32 * p + 32]
        sqk[p, 32:64] = kt[32 * p : 32 * p + 32]
    pl.semaphore_wait(barrier, greeted)
    qk_in = []
    for dy in (1, 3, 2):
        p = at_peer("seq_2", dy)
        qk_in.append(send(sqk.at[p], rqk.at[y], {"seq_2": p}))
    rqk[y] = sqk[y]
    v_in = []
    for k, dy in enumerate(ORDER):
        p = at_peer("seq_2", dy)
        loads[("wv", k)].wait()
        v = mm(xb[...], wv[k]).astype(bf16).astype(f32)
        if dy:
            sv[k] = v
            v_in.append(send(sv.at[k], rv.at[y], {"seq_2": p}))
        else:
            rv[y] = v
    loads["u"].wait()
    for p in range(N):
        us[p] = ub[:, 256 * p : 256 * p + 256].astype(f32)
    u_in = []
    for dy in (1, 3, 2):
        p = at_peer("seq_2", dy)
        u_in.append(send(us.at[p], ur.at[y], {"seq_2": p}))
    ur[y] = us[y]

    for b in range(16):
        block = xb[:, 128 * b : 128 * b + 128].astype(f32).T
        for i in range(8):
            row = 64 * (b % 4) + 16 * (i // 2)
            xt2[i % 2, b // 4, row : row + 16] = block[16 * i : 16 * i + 16]
    chunk = [lax.rem(z + i + 1, N) for i in range(N)]
    after, before = at_peer("seq_2", 1), at_peer("seq_2", 3)
    x_in = [[] for _ in range(N)]
    passing = [None] * N

    def x_start(i):
        part = chunk[i]
        mine = xg.at[part, y, c]
        x_in[i].append(send(xt2.at[1 - c, part], mine, {"batch": 1 - c}))
        same, cross = [], []
        for p in (after, before):
            same.append(send(xt2.at[c, part], mine, {"seq_2": p, "batch": c}))
            cross.append(send(xt2.at[1 - c, part], mine, {"seq_2": p, "batch": 1 - c}))
        xg[part, y, c] = xt2[c, part]
        x_in[i] += [same[1], cross[0]]
        passing[i] = (same[0], cross[1])

    def x_pass(i):
        part = chunk[i]
        up, down = passing[i]
        up.wait_recv()
        move = xg.at[part, before, c]
        x_in[i].append(send(move, move, {"seq_2": after}))
        down.wait_recv()
        move = xg.at[part, after, 1 - c]
        x_in[i].append(send(move, move, {"seq_2": before}))

    for i in range(N - 1):
        x_start(i)

    for copy in qk_in:
        copy.wait_recv()
    for h in range(2):
        lo = 16 * h
        uq = jnp.concatenate([rqk[j, lo : lo + 16] for j in range(N)], 1) * 0.5
        uk = jnp.concatenate([rqk[j, 32 + lo : 48 + lo] for j in range(N)], 1) * 0.5
        fq[h] = features(uq)
        fk[h] = features(uk)
    for copy in v_in:
        copy.wait_recv()
    ones = jnp.ones((16, TOK), bf16)
    for h in range(2):
        for j in range(N):
            vb[h, 128 * j : 128 * j + 128] = rv[j, :, 128 * h : 128 * h + 128].astype(bf16)

    def put_state(st, h, state, norm):
        st[2 * h] = state[:80]
        st[2 * h + 1] = state[80:]
        st[2 * h + 1, 73:74] = norm[:, :128]
        st[2 * h + 1, 74:75] = jnp.concatenate([norm[:, 128:], jnp.zeros((1, 96), f32)], 1)

    def get_state(pf, h):
        state = jnp.concatenate([pf[2 * h], pf[2 * h + 1]], 0)
        norm = jnp.concatenate([pf[2 * h + 1, 73:74], pf[2 * h + 1, 74:75, :32]], 1)
        return state, norm

    for h in range(2):
        put_state(st1, h, mm(fk[h], vb[h]), mm_nt(ones, fk[h])[:1])

    def scan_start(st, xr):
        copies = []
        for d in (1, 3, 2):
            p = at_peer("seq_1", d)
            copies.append(send(st.at[p], xr.at[x], {"seq_1": p}))
        xr[x] = st[x]
        return copies

    def scan_mid(copies, xr, zs, zr):
        for copy in copies:
            copy.wait_recv()
        zs[...] = (xr[0] + xr[1]) + (xr[2] + xr[3])
        return [send(zs, zr.at[z], {"seq_0": at_peer("seq_0", d)}) for d in (1, 3, 2)]

    def scan_back(copies, xr, zr, pb, pf, later):
        for copy in copies:
            copy.wait_recv()
        run = jnp.zeros((80, 128), f32)
        for d in (1, 2, 3):
            p = at_peer("seq_0", d)
            run = run + jnp.where(p > z if later else p < z, zr[p], 0.0)
        for i in reversed(range(N)) if later else range(N):
            pb[i] = run
            run = run + xr[i]
        out = []
        for d in (1, 3, 2):
            p = at_peer("seq_1", d)
            out.append(send(pb.at[p], pf.at[x], {"seq_1": p}))
        pf[x] = pb[x]
        return out

    keep = lax.broadcasted_iota(jnp.int32, (TOK, TOK), 1) >= lax.broadcasted_iota(
        jnp.int32, (TOK, TOK), 0
    )

    def local_forward(h):
        for j in range(N):
            vt[h, :, 128 * j : 128 * j + 128] = (
                rv[j, :, 128 * h : 128 * h + 128].T.astype(bf16)
            )
        scores = jnp.where(keep, mm_tn(fk[h], fq[h]), 0.0)
        dloc[h] = jnp.broadcast_to(jnp.sum(scores, 0, keepdims=True), (8, TOK))
        at[h] = scores.astype(bf16)
        num[h] = mm(vt[h], at[h])

    move = scan_start(st1, xr1)
    local_forward(0)
    move = scan_mid(move, xr1, zs1, zr1)
    local_forward(1)
    move = scan_back(move, xr1, zr1, pb1, pf1, False)
    for copy in u_in:
        copy.wait_recv()
    for h in range(2):
        for j in range(N):
            ut[h, :, 128 * j : 128 * j + 128] = ur[j, :, 128 * h : 128 * h + 128].T
    for copy in move:
        copy.wait_recv()

    for h in range(2):
        state, norm = get_state(pf1, h)
        stb[h] = state.astype(bf16)
        n_hi, n_lo = halves(norm)
        nrm[h] = jnp.concatenate([n_hi, n_lo, n_hi, jnp.zeros((5, FP), f32)], 0)
        numer = num[h] + mm_tn(stb[h], fq[h])
        denom = dloc[h, :1] + jnp.sum(mm(rows16(n_hi, n_lo), fq[h]), 0, keepdims=True)
        inverse = 1.0 / denom
        upstream = ut[h]
        g_num = upstream * inverse
        g_den = -jnp.sum(upstream * (numer * inverse), 0, keepdims=True) * inverse
        gnb[h] = g_num.astype(bf16)
        g_hi, g_lo = halves(g_den)
        gdr[h] = jnp.concatenate([g_hi, g_lo, jnp.zeros((6, TOK), f32)], 0)
        back = mm_nt(fq[h], gnb[h])
        back_norm = jnp.sum(mm_nt(rows16(g_hi, g_lo), fq[h]), 0, keepdims=True)
        put_state(st2, h, back, back_norm)

    def local_backward(h):
        g_hi, g_lo = gdr[h, 0:1], gdr[h, 1:2]
        n_hi, n_lo = nrm[h, 0:1], nrm[h, 1:2]
        inner = mm(vb[h], gnb[h]) + (g_hi + g_lo)
        ga = jnp.where(keep, inner, 0.0).astype(bf16)
        outer = mm_tn(rows16(n_hi, n_lo, n_hi), rows16(g_hi, g_hi, g_lo))
        gfq[h] = mm(fk[h], ga) + mm(stb[h], gnb[h]) + outer
        gvt[h] = mm_nt(gnb[h], at[h])
        gfk[h] = mm_nt(fq[h], ga)

    def put_grad(h, first, u, grad):
        out = (pull_back(u, grad) * 0.5).astype(bf16).astype(f32)
        for j in range(N):
            gg[c, j, first + 16 * h : first + 16 * h + 16] = out[:, 128 * j : 128 * j + 128]

    move = scan_start(st2, xr2)
    x_pass(0)
    x_start(3)
    local_backward(0)
    move = scan_mid(move, xr2, zs2, zr2)
    x_pass(1)
    local_backward(1)
    move = scan_back(move, xr2, zr2, pb2, pf2, True)
    for h in range(2):
        lo = 16 * h
        uq = jnp.concatenate([rqk[j, lo : lo + 16] for j in range(N)], 1) * 0.5
        put_grad(h, 256, uq, gfq[h])
    for copy in move:
        copy.wait_recv()
    first16 = lax.broadcasted_iota(jnp.int32, (16, TOK), 0) < 2
    flag = jnp.where(first16, 1.0, 0.0).astype(bf16)
    for h in range(2):
        back, back_norm = get_state(pf2, h)
        backb = back.astype(bf16)
        b_hi, b_lo = halves(back_norm)
        g_val = gvt[h] + mm_tn(backb, fk[h])
        g_val = g_val.astype(bf16).astype(f32)
        for j in range(N):
            gg[c, j, 128 * h : 128 * h + 128] = g_val[:, 128 * j : 128 * j + 128]
        g_fk = gfk[h] + mm(backb, vt[h]) + mm_tn(rows16(b_hi, b_lo), flag)
        lo = 32 + 16 * h
        uk = jnp.concatenate([rqk[j, lo : lo + 16] for j in range(N)], 1) * 0.5
        put_grad(h, 288, uk, g_fk)

    pair_g = send(gg.at[c], gg.at[c], {"batch": 1 - c})
    x_pass(2)
    pair_g.wait_recv()
    rhs = jnp.concatenate([gg[i, j].astype(bf16) for j in range(N) for i in range(2)], 1)

    a_in, b_in = [], []

    def weights_of(i):
        part = chunk[i]
        for copy in x_in[i]:
            copy.wait_recv()
        lhs = jnp.concatenate(
            [xg[part, j, k].astype(bf16) for j in range(N) for k in range(2)], 1
        )
        out = mm_nt(lhs, rhs)
        for xx in range(N):
            for j in range(N):
                own = out[64 * xx + 16 * j : 64 * xx + 16 * j + 16]
                thin = own[:, 256:320]
                da[i, xx, 24 * j : 24 * j + 16] = own[:, :128]
                da[i, xx, 24 * j + 16 : 24 * j + 24] = jnp.concatenate([thin[:8], thin[8:]], 1)
                db[i, xx, 16 * j : 16 * j + 16] = own[:, 128:256]
        a_in.append([])
        for k, d in enumerate((1, 3, 2)):
            p = at_peer("seq_1", d)
            a_in[i].append(send(da.at[i, p], ra.at[i, k], {"seq_1": p}))
        if i < N - 1:
            b_in.append(send(db.at[i], rb.at[i], {"seq_0": part}))

    last = []

    def a_onward(i):
        for copy in a_in[i]:
            copy.wait_recv()
        total = (da[i, x] + ra[i, 0]) + (ra[i, 1] + ra[i, 2])
        for j in range(N):
            sa[i, j] = total[24 * j : 24 * j + 24]
        for dy in ORDER:
            p = at_peer("seq_2", dy)
            target = {"seq_2": p}
            if i < N - 1:
                target["seq_0"] = chunk[i]
            elif dy == 0:
                fa[i, y] = sa[i, y]
                continue
            last.append(send(sa.at[i, p], fa.at[i, y], target))

    weights_of(0)
    weights_of(1)
    a_onward(0)
    weights_of(2)
    x_pass(3)
    g_in = []
    for dy in (1, 3, 2):
        p = at_peer("seq_2", dy)
        g_in.append(send(gg.at[c, p], gb.at[y], {"seq_2": p}))
    gb[y] = gg[c, y]
    a_onward(1)
    a_onward(2)
    weights_of(3)
    for copy in b_in:
        copy.wait_recv()
    for xx in range(N):
        db[3, xx] = (db[3, xx] + rb[0, xx]) + (rb[1, xx] + rb[2, xx])
    for d in ORDER:
        px = at_peer("seq_1", d)
        for dy in ORDER:
            p = at_peer("seq_2", dy)
            piece = db.at[3, px, pl.ds(pl.multiple_of(p * 16, 16), 16)]
            if d or dy:
                last.append(send(piece, fb.at[d, y], {"seq_1": px, "seq_2": p}))
            else:
                fb[0, y] = piece[...]
    a_onward(3)

    for copy in g_in:
        copy.wait_recv()
    g_q = jnp.concatenate([gb[j, 256:288] for j in range(N)], 0).T.astype(bf16)
    g_k = jnp.concatenate([gb[j, 288:320] for j in range(N)], 0).T.astype(bf16)
    g_v = []
    for k, dy in enumerate(ORDER):
        p = at_peer("seq_2", dy)
        g_v.append(gb[p, 0:256].T.astype(bf16))

    def inputs_of(i, carry):
        rows = pl.ds(pl.multiple_of(i * 512, 512), 512)
        acc = mm_nt(g_q, wq[rows]) + mm_nt(g_k, wk[rows])
        for k in range(N):
            acc = acc + mm_nt(g_v[k], wv[k, rows])
        gi[:, rows] = acc.astype(bf16)
        return carry

    lax.fori_loop(0, N, inputs_of, 0)
    out_copy = pltpu.make_async_copy(gi, gin.at[0], osem)
    out_copy.start()
    for copy in last:
        copy.wait_recv()
    for p in range(N):
        both = (fa[0, p] + fa[1, p]) + (fa[2, p] + fa[3, p])
        res[p, 0:16] = both[:16]
        res[p, 16:32] = (fb[0, p] + fb[1, p]) + (fb[2, p] + fb[3, p])
        res[p, 32:40] = both[16:]
    out_copy.wait()
    assert used[0] == SENDS
    for copy in started:
        copy.wait_send()


def finish(gin_ref, res_ref, gin_out, gwq, gwk, gwv):
    gin_out[...] = gin_ref[...]
    lane = lax.broadcasted_iota(jnp.int32, (16, 128), 1) // 32
    w_q = jnp.zeros((16, 128), f32)
    w_k = jnp.zeros((16, 128), f32)
    for p in range(N):
        gwv[:, 256 * p : 256 * p + 128] = res_ref[p, 0:16]
        gwv[:, 256 * p + 128 : 256 * p + 256] = res_ref[p, 16:32]
        thin = res_ref[p, 32:40]
        thin = jnp.concatenate([thin, pltpu.roll(thin, 64, 1)], 0)
        from_q = pltpu.roll(thin, 32 * p, 1) if p else thin
        w_q = jnp.where(lane == p, from_q, w_q)
        from_k = pltpu.roll(thin, (32 * p + 96) % 128, 1) if p != 1 else thin
        w_k = jnp.where(lane == p, from_k, w_k)
    gwq[...] = w_q
    gwk[...] = w_k


SENDS = 3 + 3 + 3 + 18 + 1 + 4 * 7 + 3 + 12 + 3 + 15 + 15


def body(inputs, cotangent, w_query, w_key, w_value):
    vmem = pltpu.VMEM
    hbm = pl.BlockSpec(memory_space=pl.ANY)
    here = pl.BlockSpec(memory_space=pltpu.VMEM)
    scan = [
        vmem((4, 80, 128), f32), vmem((4, 80, 128), f32), vmem((80, 128), f32),
        vmem((4, 80, 128), f32), vmem((4, 80, 128), f32), vmem((4, 80, 128), f32),
    ]
    scratch = [
        vmem((BLK, D), bf16), vmem((BLK, 1024), bf16), vmem((D, 128), bf16), vmem((D, 128), bf16),
        vmem((4, D, 256), bf16), vmem((2, 4, 256, 128), f32), vmem((4, 4, 2, 256, 128), f32),
        vmem((4, 64, 128), f32), vmem((3, 128, 256), f32), vmem((4, 64, 128), f32),
        vmem((4, 128, 256), f32), vmem((4, 128, 256), f32), vmem((4, 128, 256), f32),
        vmem((2, FP, TOK), bf16), vmem((2, FP, TOK), bf16), vmem((2, TOK, 128), bf16),
        vmem((2, 128, TOK), bf16), vmem((2, 128, TOK), f32), vmem((2, TOK, TOK), bf16),
        vmem((2, 128, TOK), f32), vmem((2, 8, TOK), f32), vmem((2, 128, TOK), bf16),
        vmem((2, 8, TOK), f32), vmem((2, FP, TOK), f32), vmem((2, FP, TOK), f32),
        vmem((2, 128, TOK), f32), vmem((2, FP, 128), bf16), vmem((2, 8, FP), f32),
        *scan, *scan,
        vmem((2, 4, 320, 128), f32), vmem((4, 320, 128), f32), vmem((BLK, D), bf16),
        vmem((4, 4, 96, 128), f32), vmem((4, 4, 64, 128), f32),
        vmem((4, 3, 96, 128), f32), vmem((3, 4, 64, 128), f32),
        vmem((4, 4, 24, 128), f32), vmem((4, 4, 24, 128), f32), vmem((4, 4, 16, 128), f32),
        pltpu.SemaphoreType.DMA((8,)), pltpu.SemaphoreType.DMA, pltpu.SemaphoreType.DMA((SENDS,)),
        pltpu.SemaphoreType.DMA((SENDS,)),
    ]
    gin, res = pl.pallas_call(
        kernel,
        out_shape=(
            jax.ShapeDtypeStruct((1, BLK, D), bf16),
            jax.ShapeDtypeStruct((4, 40, 128), f32),
        ),
        in_specs=[hbm] * 5,
        out_specs=(hbm, here),
        scratch_shapes=scratch,
        compiler_params=pltpu.CompilerParams(
            collective_id=0, has_side_effects=True, vmem_limit_bytes=60 * 1024 * 1024
        ),
    )(inputs, cotangent, w_query, w_key, w_value)
    return pl.pallas_call(
        finish,
        out_shape=(
            jax.ShapeDtypeStruct((1, BLK, D), bf16),
            jax.ShapeDtypeStruct((16, 128), f32),
            jax.ShapeDtypeStruct((16, 128), f32),
            jax.ShapeDtypeStruct((16, 1024), f32),
        ),
        in_specs=[here] * 2,
        out_specs=(here,) * 4,
    )(gin, res)


def solution(mesh):
    split = Mesh(
        mesh.devices.reshape(4, 4, 4, mesh.shape["batch"]), ("seq_0", "seq_1", "seq_2", "batch")
    )
    in_specs = (P("batch", SEQ, None), P("batch", SEQ, None), P(), P(), P())
    out_specs = (P("batch", SEQ, None), P(SEQ_BATCH, None), P(SEQ_BATCH, None), P(SEQ_BATCH, None))
    return jax.shard_map(body, mesh=split, in_specs=in_specs, out_specs=out_specs, check_vma=False)
```

```python
import math

import jax
import jax.numpy as jnp
from jax import lax
from jax.experimental import pallas as pl
from jax.experimental.pallas import tpu as pltpu
from jax.sharding import Mesh
from jax.sharding import PartitionSpec as P

D = 2048
H = 8
DK = 16
DV = 128
SEQ = ("seq_0", "seq_1", "seq_2")
SEQ_BATCH = ("seq_0", "seq_1", "seq_2", "batch")
N = 4
BLK = 128
TOK = N * BLK
FP = 160
ROOT = 1.0 / math.sqrt(2.0)
ORDER = (1, 3, 2, 0)
f32 = jnp.float32
bf16 = jnp.bfloat16
MESH_ID = pl.DeviceIdType.MESH


def mm(a, b):
    return lax.dot_general(a, b, (((1,), (0,)), ((), ())), preferred_element_type=f32)


def mm_nt(a, b):
    return lax.dot_general(a, b, (((1,), (1,)), ((), ())), preferred_element_type=f32)


def mm_tn(a, b):
    return lax.dot_general(a, b, (((0,), (0,)), ((), ())), preferred_element_type=f32)


def halves(row):
    high = row.astype(bf16).astype(f32)
    return high, row - high


def rows16(*rows):
    n = rows[0].shape[1]
    at = lax.broadcasted_iota(jnp.int32, (16, n), 0)
    out = jnp.zeros((16, n), f32)
    for i, row in enumerate(rows):
        out = jnp.where(at == i, jnp.broadcast_to(row, (16, n)), out)
    return out.astype(bf16)


def turned(u, d):
    d = d % DK
    return u if d == 0 else pltpu.roll(u, DK - d, 0)


def features(u):
    n = u.shape[1]
    parts = [u, u * u * ROOT]
    for d in range(1, 8):
        parts.append(u * turned(u, d))
    parts.append(u[:8] * u[8:])
    first = lax.broadcasted_iota(jnp.int32, (8, n), 0) == 0
    parts.append(jnp.where(first, 1.0, 0.0).astype(f32))
    return jnp.concatenate(parts, 0).astype(bf16)


def pull_back(u, g):
    out = g[0:16] + (g[16:32] * (2.0 * ROOT)) * u
    for d in range(1, 8):
        pair = g[16 + 16 * d : 32 + 16 * d]
        out = out + pair * turned(u, d) + turned(pair * u, -d)
    pair = g[144:152]
    return out + jnp.concatenate([pair * u[8:], pair * u[:8]], 0)


def kernel(
    x_hbm, u_hbm, wq_hbm, wk_hbm, wv_hbm,
    gin, res,
    xb, ub, wq, wk, wv, xt2, xg,
    sqk, sv, rqk, rv, us, ur,
    fq, fk, vb, vt, ut, at, num, dloc, gnb, gdr, gfq, gfk, gvt, stb, nrm,
    st1, xr1, zs1, zr1, pb1, pf1,
    st2, xr2, zs2, zr2, pb2, pf2,
    gg, gb, gi, gacc, da, db, ra, rb, sa, fa, fb, rs, total,
    lsem, osem, rsm, ssem, rsem,
):
    z, x, y, c = (lax.axis_index(a) for a in SEQ_BATCH)
    place = {"seq_0": z, "seq_1": x, "seq_2": y}
    bytes_sent, groups = [0], [0]

    class Group:
        def __init__(self, like):
            self.like, self.k = like, groups[0]
            groups[0] += 1

        def copy(self, src, dst, target):
            return pltpu.make_async_remote_copy(
                src_ref=src, dst_ref=dst, send_sem=ssem, recv_sem=rsem.at[self.k],
                device_id=target, device_id_type=MESH_ID,
            )

        def send(self, src, dst, target):
            bytes_sent[0] += math.prod(src.shape) * 4
            self.copy(src, dst, target).start()

        def wait(self):
            self.copy(self.like, self.like, {"batch": 1 - c}).wait_recv()

    def one(src, dst, target):
        group = Group(dst)
        group.send(src, dst, target)
        return group

    def slot(place, j):
        return lax.rem(place - j + 7, N)

    def at_peer(axis, d):
        return lax.rem(place[axis] + d, N)

    loads = {}

    def load(name, k, src, dst):
        loads[name] = pltpu.make_async_copy(src, dst, lsem.at[k])
        loads[name].start()

    load("x", 0, x_hbm.at[0], xb)
    load("wq", 1, wq_hbm, wq)
    load("wk", 2, wk_hbm, wk)
    for k, dy in enumerate(ORDER):
        cols = pl.ds(pl.multiple_of(at_peer("seq_2", dy) * 256, 256), 256)
        load(("wv", k), 3 + k, wv_hbm.at[:, cols], wv.at[k])
    load("u", 7, u_hbm.at[0], ub)

    barrier = pltpu.get_barrier_semaphore()
    greeted = 0
    for d in range(N):
        for e in range(N):
            pairs = [("seq_0", "seq_2")] if d or e else []
            if d:
                pairs.append(("seq_1", "seq_2"))
            for first, second in pairs:
                greeted += 1
                pl.semaphore_signal(
                    barrier, inc=1, device_id_type=MESH_ID,
                    device_id={first: at_peer(first, d), second: at_peer(second, e)},
                )
        greeted += 1
        pl.semaphore_signal(
            barrier, inc=1, device_id_type=MESH_ID,
            device_id={"seq_2": at_peer("seq_2", d), "batch": 1 - c},
        )

    loads["x"].wait()
    loads["wq"].wait()
    qt = mm(xb[...], wq[...]).T
    loads["wk"].wait()
    kt = mm(xb[...], wk[...]).T
    for p in range(N):
        sqk[p, 0:32] = qt[32 * p : 32 * p + 32]
        sqk[p, 32:64] = kt[32 * p : 32 * p + 32]
    pl.semaphore_wait(barrier, greeted)
    qk_in = Group(rqk.at[pl.ds(0, 3)])
    for dy in (1, 3, 2):
        p = at_peer("seq_2", dy)
        qk_in.send(sqk.at[p], rqk.at[dy - 1], {"seq_2": p})
    rqk[3] = sqk[y]
    v_in = Group(rv.at[pl.ds(0, 3)])
    for k, dy in enumerate(ORDER):
        p = at_peer("seq_2", dy)
        loads[("wv", k)].wait()
        v = mm(xb[...], wv[k]).astype(bf16).astype(f32)
        if dy:
            sv[k] = v
            v_in.send(sv.at[k], rv.at[dy - 1], {"seq_2": p})
        else:
            rv[3] = v
    loads["u"].wait()
    for p in range(N):
        us[p] = ub[:, 256 * p : 256 * p + 256].astype(f32)
    u_in = Group(ur.at[pl.ds(0, 3)])
    for dy in (1, 3, 2):
        p = at_peer("seq_2", dy)
        u_in.send(us.at[p], ur.at[dy - 1], {"seq_2": p})
    ur[3] = us[y]

    for b in range(16):
        block = xb[:, 128 * b : 128 * b + 128].astype(f32).T
        for i in range(8):
            row = 64 * (b % 4) + 16 * (i // 2)
            xt2[i % 2, b // 4, row : row + 16] = block[16 * i : 16 * i + 16]
    chunk = [lax.rem(z + i + 1, N) for i in range(N)]
    after, before = at_peer("seq_2", 1), at_peer("seq_2", 3)
    x_in = [Group(xg.at[i, pl.ds(0, 5)]) for i in range(N)]
    passing = [None] * N

    def x_start(i):
        part = chunk[i]
        mine = xg.at[part, 2 * y + c]
        x_in[i].send(xt2.at[1 - c, part], mine, {"batch": 1 - c})
        up = one(xt2.at[c, part], mine, {"seq_2": after, "batch": c})
        x_in[i].send(xt2.at[c, part], mine, {"seq_2": before, "batch": c})
        x_in[i].send(xt2.at[1 - c, part], mine, {"seq_2": after, "batch": 1 - c})
        down = one(xt2.at[1 - c, part], mine, {"seq_2": before, "batch": 1 - c})
        xg[part, 2 * y + c] = xt2[c, part]
        passing[i] = (up, down)

    def x_pass(i):
        part = chunk[i]
        up, down = passing[i]
        up.wait()
        move = xg.at[part, 2 * before + c]
        x_in[i].send(move, move, {"seq_2": after})
        down.wait()
        move = xg.at[part, 2 * after + 1 - c]
        x_in[i].send(move, move, {"seq_2": before})

    for i in range(N - 1):
        x_start(i)

    qk_in.wait()
    for h in range(2):
        lo = 16 * h
        uq = jnp.concatenate([rqk[slot(y, j), lo : lo + 16] for j in range(N)], 1) * 0.5
        uk = jnp.concatenate([rqk[slot(y, j), 32 + lo : 48 + lo] for j in range(N)], 1) * 0.5
        fq[h] = features(uq)
        fk[h] = features(uk)
    v_in.wait()
    ones = jnp.ones((16, TOK), bf16)
    for h in range(2):
        for j in range(N):
            vb[h, 128 * j : 128 * j + 128] = rv[slot(y, j), :, 128 * h : 128 * h + 128].astype(bf16)

    def put_state(st, h, state, norm):
        st[2 * h] = state[:80]
        st[2 * h + 1] = state[80:]
        st[2 * h + 1, 73:74] = norm[:, :128]
        st[2 * h + 1, 74:75] = jnp.concatenate([norm[:, 128:], jnp.zeros((1, 96), f32)], 1)

    def get_state(pf, h):
        low, high = slot(x, 2 * h), slot(x, 2 * h + 1)
        state = jnp.concatenate([pf[low], pf[high]], 0)
        norm = jnp.concatenate([pf[high, 73:74], pf[high, 74:75, :32]], 1)
        return state, norm

    for h in range(2):
        put_state(st1, h, mm(fk[h], vb[h]), mm_nt(ones, fk[h])[:1])

    def scan_start(st, xr):
        group = Group(xr.at[pl.ds(0, 3)])
        for d in (1, 3, 2):
            p = at_peer("seq_1", d)
            group.send(st.at[p], xr.at[d - 1], {"seq_1": p})
        xr[3] = st[x]
        return group

    def scan_mid(group, xr, zs, zr):
        group.wait()
        zs[...] = (xr[0] + xr[1]) + (xr[2] + xr[3])
        group = Group(zr)
        for d in (1, 3, 2):
            group.send(zs, zr.at[d - 1], {"seq_0": at_peer("seq_0", d)})
        return group

    def scan_back(group, xr, zr, pb, pf, later):
        group.wait()
        run = jnp.zeros((80, 128), f32)
        for d in (1, 2, 3):
            run = run + jnp.where(z < d if later else z >= d, zr[d - 1], 0.0)
        for i in reversed(range(N)) if later else range(N):
            pb[i] = run
            run = run + xr[slot(x, i)]
        group = Group(pf.at[pl.ds(0, 3)])
        for d in (1, 3, 2):
            p = at_peer("seq_1", d)
            group.send(pb.at[p], pf.at[d - 1], {"seq_1": p})
        pf[3] = pb[x]
        return group

    keep = lax.broadcasted_iota(jnp.int32, (TOK, TOK), 1) >= lax.broadcasted_iota(
        jnp.int32, (TOK, TOK), 0
    )

    def local_forward(h):
        for j in range(N):
            vt[h, :, 128 * j : 128 * j + 128] = (
                rv[slot(y, j), :, 128 * h : 128 * h + 128].T.astype(bf16)
            )
        scores = jnp.where(keep, mm_tn(fk[h], fq[h]), 0.0)
        dloc[h] = jnp.broadcast_to(jnp.sum(scores, 0, keepdims=True), (8, TOK))
        at[h] = scores.astype(bf16)
        num[h] = mm(vt[h], at[h])

    move = scan_start(st1, xr1)
    local_forward(0)
    move = scan_mid(move, xr1, zs1, zr1)
    local_forward(1)
    move = scan_back(move, xr1, zr1, pb1, pf1, False)
    u_in.wait()
    for h in range(2):
        for j in range(N):
            ut[h, :, 128 * j : 128 * j + 128] = ur[slot(y, j), :, 128 * h : 128 * h + 128].T
    move.wait()

    for h in range(2):
        state, norm = get_state(pf1, h)
        stb[h] = state.astype(bf16)
        n_hi, n_lo = halves(norm)
        nrm[h] = jnp.concatenate([n_hi, n_lo, n_hi, jnp.zeros((5, FP), f32)], 0)
        numer = num[h] + mm_tn(stb[h], fq[h])
        denom = dloc[h, :1] + jnp.sum(mm(rows16(n_hi, n_lo), fq[h]), 0, keepdims=True)
        inverse = 1.0 / denom
        upstream = ut[h]
        g_num = upstream * inverse
        g_den = -jnp.sum(upstream * (numer * inverse), 0, keepdims=True) * inverse
        gnb[h] = g_num.astype(bf16)
        g_hi, g_lo = halves(g_den)
        gdr[h] = jnp.concatenate([g_hi, g_lo, jnp.zeros((6, TOK), f32)], 0)
        back = mm_nt(fq[h], gnb[h])
        back_norm = jnp.sum(mm_nt(rows16(g_hi, g_lo), fq[h]), 0, keepdims=True)
        put_state(st2, h, back, back_norm)

    def local_backward(h):
        g_hi, g_lo = gdr[h, 0:1], gdr[h, 1:2]
        n_hi, n_lo = nrm[h, 0:1], nrm[h, 1:2]
        inner = mm(vb[h], gnb[h]) + (g_hi + g_lo)
        ga = jnp.where(keep, inner, 0.0).astype(bf16)
        outer = mm_tn(rows16(n_hi, n_lo, n_hi), rows16(g_hi, g_hi, g_lo))
        gfq[h] = mm(fk[h], ga) + mm(stb[h], gnb[h]) + outer
        gvt[h] = mm_nt(gnb[h], at[h])
        gfk[h] = mm_nt(fq[h], ga)

    def put_grad(h, first, u, grad):
        out = (pull_back(u, grad) * 0.5).astype(bf16).astype(f32)
        for j in range(N):
            gg[c, j, first + 16 * h : first + 16 * h + 16] = out[:, 128 * j : 128 * j + 128]

    move = scan_start(st2, xr2)
    x_pass(0)
    x_start(3)
    local_backward(0)
    move = scan_mid(move, xr2, zs2, zr2)
    x_pass(1)
    local_backward(1)
    move = scan_back(move, xr2, zr2, pb2, pf2, True)
    for h in range(2):
        lo = 16 * h
        uq = jnp.concatenate([rqk[slot(y, j), lo : lo + 16] for j in range(N)], 1) * 0.5
        put_grad(h, 256, uq, gfq[h])
    move.wait()
    first16 = lax.broadcasted_iota(jnp.int32, (16, TOK), 0) < 2
    flag = jnp.where(first16, 1.0, 0.0).astype(bf16)
    for h in range(2):
        back, back_norm = get_state(pf2, h)
        backb = back.astype(bf16)
        b_hi, b_lo = halves(back_norm)
        g_val = gvt[h] + mm_tn(backb, fk[h])
        g_val = g_val.astype(bf16).astype(f32)
        for j in range(N):
            gg[c, j, 128 * h : 128 * h + 128] = g_val[:, 128 * j : 128 * j + 128]
        g_fk = gfk[h] + mm(backb, vt[h]) + mm_tn(rows16(b_hi, b_lo), flag)
        lo = 32 + 16 * h
        uk = jnp.concatenate([rqk[slot(y, j), lo : lo + 16] for j in range(N)], 1) * 0.5
        put_grad(h, 288, uk, g_fk)

    pair_g = one(gg.at[c], gg.at[c], {"batch": 1 - c})
    x_pass(2)
    def gin_add(k, fresh):
        g_v = gb[(3 - ORDER[k]) % 4, 0:256].T.astype(bf16)

        def columns(i, carry):
            rows = pl.ds(pl.multiple_of(i * 512, 512), 512)
            part = mm_nt(g_v, wv[k, rows])
            gacc[:, rows] = part if fresh else gacc[:, rows] + part
            return carry

        lax.fori_loop(0, N, columns, 0)

    gb[3] = gg[c, y]
    gin_add(3, True)
    x_pass(3)
    g_thin = Group(gb.at[pl.ds(0, 3), pl.ds(256, 64)])
    g_wide = {}
    for dy in (2, 1, 3):
        p = at_peer("seq_2", dy)
        g_thin.send(gg.at[c, p, pl.ds(256, 64)], gb.at[dy - 1, pl.ds(256, 64)], {"seq_2": p})
    for dy in (2, 1, 3):
        p = at_peer("seq_2", dy)
        g_wide[dy] = one(gg.at[c, p, pl.ds(0, 256)], gb.at[dy - 1, pl.ds(0, 256)], {"seq_2": p})
    pair_g.wait()
    rhs = jnp.concatenate([gg[i, j].astype(bf16) for j in range(N) for i in range(2)], 1)

    a_in = [Group(ra.at[i]) for i in range(N)]
    b_in = Group(rb)

    def weights_of(i):
        part = chunk[i]
        x_in[i].wait()
        lhs = jnp.concatenate(
            [xg[part, j].astype(bf16) for j in range(8)], 1
        )
        out = mm_nt(lhs, rhs)
        for xx in range(N):
            for j in range(N):
                own = out[64 * xx + 16 * j : 64 * xx + 16 * j + 16]
                thin = own[:, 256:320]
                da[i, xx, 24 * j : 24 * j + 16] = own[:, :128]
                da[i, xx, 24 * j + 16 : 24 * j + 24] = jnp.concatenate([thin[:8], thin[8:]], 1)
                db[i, xx, 16 * j : 16 * j + 16] = own[:, 128:256]
        for k, d in enumerate((1, 3, 2)):
            p = at_peer("seq_1", d)
            a_in[i].send(da.at[i, p], ra.at[i, k], {"seq_1": p})
        if i < N - 1:
            b_in.send(db.at[i], rb.at[i], {"seq_0": part})

    a_last, b_last = Group(fa.at[pl.ds(0, 15)]), Group(fb.at[pl.ds(0, 15)])

    def a_onward(i):
        a_in[i].wait()
        total = (da[i, x] + ra[i, 0]) + (ra[i, 1] + ra[i, 2])
        for j in range(N):
            sa[i, j] = total[24 * j : 24 * j + 24]
        for dy in ORDER:
            p = at_peer("seq_2", dy)
            target = {"seq_2": p}
            if i < N - 1:
                target["seq_0"] = chunk[i]
            elif dy == 0:
                fa[15] = sa[i, y]
                continue
            a_last.send(sa.at[i, p], fa.at[4 * i + (dy + 3) % 4], target)

    weights_of(0)
    weights_of(1)
    a_onward(0)
    weights_of(2)
    weights_of(3)
    b_in.wait()
    for xx in range(N):
        db[3, xx] = (db[3, xx] + rb[0, xx]) + (rb[1, xx] + rb[2, xx])
    for d in ORDER:
        px = at_peer("seq_1", d)
        for dy in ORDER:
            p = at_peer("seq_2", dy)
            piece = db.at[3, px, pl.ds(pl.multiple_of(p * 16, 16), 16)]
            if d or dy:
                into = fb.at[4 * ((d + 3) % 4) + (dy + 3) % 4]
                b_last.send(piece, into, {"seq_1": px, "seq_2": p})
            else:
                fb[15] = piece[...]
    a_onward(1)
    a_onward(2)

    g_thin.wait()
    g_q = jnp.concatenate([gb[slot(y, j), 256:288] for j in range(N)], 0).T.astype(bf16)
    g_k = jnp.concatenate([gb[slot(y, j), 288:320] for j in range(N)], 0).T.astype(bf16)

    def thin_columns(i, carry):
        rows = pl.ds(pl.multiple_of(i * 512, 512), 512)
        gacc[:, rows] = gacc[:, rows] + (mm_nt(g_q, wq[rows]) + mm_nt(g_k, wk[rows]))
        return carry

    lax.fori_loop(0, N, thin_columns, 0)
    a_onward(3)
    g_wide[1].wait()
    gin_add(1, False)
    g_wide[3].wait()
    gin_add(0, False)
    g_wide[2].wait()
    g_v = gb[1, 0:256].T.astype(bf16)

    def inputs_of(i, carry):
        rows = pl.ds(pl.multiple_of(i * 512, 512), 512)
        gi[:, rows] = (gacc[:, rows] + mm_nt(g_v, wv[2, rows])).astype(bf16)
        return carry

    lax.fori_loop(0, N, inputs_of, 0)
    out_copy = pltpu.make_async_copy(gi, gin.at[0], osem)
    out_copy.start()
    a_last.wait()
    b_last.wait()
    for dy in range(N):
        p = at_peer("seq_2", (4 - dy) % 4)
        k = (dy + 3) % 4
        both = (fa[k] + fa[4 + k]) + (fa[8 + k] + fa[12 + k])
        rs[p, 0:16] = both[:16]
        rs[p, 16:32] = (fb[k] + fb[4 + k]) + (fb[8 + k] + fb[12 + k])
        rs[p, 32:40] = both[16:]
    res_copy = pltpu.make_async_copy(rs, res, rsm)
    res_copy.start()
    out_copy.wait()
    res_copy.wait()
    assert groups[0] == GROUPS and bytes_sent[0] == SENT * 512
    group = Group(None)
    group.k = 0
    group.copy(total, total, {"batch": 1 - c}).wait_send()


def finish(gin_ref, res_hbm, gin_out, gwq, gwk, gwv, res_ref, sems):
    copy = pltpu.make_async_copy(gin_ref, gin_out, sems.at[0])
    copy.start()
    fetch = pltpu.make_async_copy(res_hbm, res_ref, sems.at[1])
    fetch.start()
    fetch.wait()
    lane = lax.broadcasted_iota(jnp.int32, (16, 128), 1) // 32
    w_q = jnp.zeros((16, 128), f32)
    w_k = jnp.zeros((16, 128), f32)
    for p in range(N):
        gwv[:, 256 * p : 256 * p + 128] = res_ref[p, 0:16]
        gwv[:, 256 * p + 128 : 256 * p + 256] = res_ref[p, 16:32]
        thin = res_ref[p, 32:40]
        thin = jnp.concatenate([thin, pltpu.roll(thin, 64, 1)], 0)
        from_q = pltpu.roll(thin, 32 * p, 1) if p else thin
        w_q = jnp.where(lane == p, from_q, w_q)
        from_k = pltpu.roll(thin, (32 * p + 96) % 128, 1) if p != 1 else thin
        w_k = jnp.where(lane == p, from_k, w_k)
    gwq[...] = w_q
    gwk[...] = w_k
    copy.wait()


GROUPS = 3 + 6 + 4 * 3 + 1 + 4 + 4 + 1 + 2
SENT = (
    3 * 64 + 6 * 256 + 18 * 80 + 28 * 256 + 4 * 320 + 3 * 320
    + 12 * 96 + 12 * 64 + 15 * 24 + 15 * 16
)


def body(inputs, cotangent, w_query, w_key, w_value):
    vmem = pltpu.VMEM
    hbm = pl.BlockSpec(memory_space=pl.ANY)
    here = pl.BlockSpec(memory_space=pltpu.VMEM)
    scan = [
        vmem((4, 80, 128), f32), vmem((4, 80, 128), f32), vmem((80, 128), f32),
        vmem((3, 80, 128), f32), vmem((4, 80, 128), f32), vmem((4, 80, 128), f32),
    ]
    scratch = [
        vmem((BLK, D), bf16), vmem((BLK, 1024), bf16), vmem((D, 128), bf16), vmem((D, 128), bf16),
        vmem((4, D, 256), bf16), vmem((2, 4, 256, 128), f32), vmem((4, 8, 256, 128), f32),
        vmem((4, 64, 128), f32), vmem((3, 128, 256), f32), vmem((4, 64, 128), f32),
        vmem((4, 128, 256), f32), vmem((4, 128, 256), f32), vmem((4, 128, 256), f32),
        vmem((2, FP, TOK), bf16), vmem((2, FP, TOK), bf16), vmem((2, TOK, 128), bf16),
        vmem((2, 128, TOK), bf16), vmem((2, 128, TOK), f32), vmem((2, TOK, TOK), bf16),
        vmem((2, 128, TOK), f32), vmem((2, 8, TOK), f32), vmem((2, 128, TOK), bf16),
        vmem((2, 8, TOK), f32), vmem((2, FP, TOK), f32), vmem((2, FP, TOK), f32),
        vmem((2, 128, TOK), f32), vmem((2, FP, 128), bf16), vmem((2, 8, FP), f32),
        *scan, *scan,
        vmem((2, 4, 320, 128), f32), vmem((4, 320, 128), f32), vmem((BLK, D), bf16),
        vmem((BLK, D), f32), vmem((4, 4, 96, 128), f32), vmem((4, 4, 64, 128), f32),
        vmem((4, 3, 96, 128), f32), vmem((3, 4, 64, 128), f32),
        vmem((4, 4, 24, 128), f32), vmem((16, 24, 128), f32), vmem((16, 16, 128), f32),
        vmem((4, 40, 128), f32), vmem((SENT, 128), f32),
        pltpu.SemaphoreType.DMA((8,)), pltpu.SemaphoreType.DMA, pltpu.SemaphoreType.DMA, pltpu.SemaphoreType.DMA,
        pltpu.SemaphoreType.DMA((GROUPS,)),
    ]
    gin, res = pl.pallas_call(
        kernel,
        out_shape=(
            pltpu.VMEM((1, BLK, D), bf16),
            pltpu.VMEM((4, 40, 128), f32),
        ),
        in_specs=[pl.BlockSpec(memory_space=pltpu.HBM)] * 5,
        out_specs=(hbm, hbm),
        scratch_shapes=scratch,
        compiler_params=pltpu.CompilerParams(
            collective_id=0, has_side_effects=True, vmem_limit_bytes=60 * 1024 * 1024
        ),
    )(inputs, cotangent, w_query, w_key, w_value)
    return pl.pallas_call(
        finish,
        out_shape=(
            jax.ShapeDtypeStruct((1, BLK, D), bf16),
            jax.ShapeDtypeStruct((16, 128), f32),
            jax.ShapeDtypeStruct((16, 128), f32),
            jax.ShapeDtypeStruct((16, 1024), f32),
        ),
        in_specs=[hbm] * 2,
        out_specs=(pl.BlockSpec(memory_space=pltpu.HBM), here, here, here),
        scratch_shapes=[pltpu.VMEM((4, 40, 128), f32), pltpu.SemaphoreType.DMA((2,))],
        compiler_params=pltpu.CompilerParams(vmem_limit_bytes=4 * 1024 * 1024),
    )(gin, res)


def solution(mesh):
    split = Mesh(
        mesh.devices.reshape(4, 4, 4, mesh.shape["batch"]), ("seq_0", "seq_1", "seq_2", "batch")
    )
    in_specs = (P("batch", SEQ, None), P("batch", SEQ, None), P(), P(), P())
    out_specs = (P("batch", SEQ, None), P(SEQ_BATCH, None), P(SEQ_BATCH, None), P(SEQ_BATCH, None))
    return jax.shard_map(body, mesh=split, in_specs=in_specs, out_specs=out_specs, check_vma=False)
```

```python
import math

import jax
import jax.numpy as jnp
from jax import lax
from jax.experimental import pallas as pl
from jax.experimental.pallas import tpu as pltpu
from jax.sharding import Mesh
from jax.sharding import PartitionSpec as P

D = 2048
H = 8
DK = 16
DV = 128
SEQ = ("seq_0", "seq_1", "seq_2")
SEQ_BATCH = ("seq_0", "seq_1", "seq_2", "batch")
N = 4
BLK = 128
TOK = N * BLK
FP = 160
ROOT = 1.0 / math.sqrt(2.0)
ORDER = (1, 3, 2, 0)
f32 = jnp.float32
bf16 = jnp.bfloat16
MESH_ID = pl.DeviceIdType.MESH


def mm(a, b):
    return lax.dot_general(a, b, (((1,), (0,)), ((), ())), preferred_element_type=f32)


def mm_nt(a, b):
    return lax.dot_general(a, b, (((1,), (1,)), ((), ())), preferred_element_type=f32)


def mm_tn(a, b):
    return lax.dot_general(a, b, (((0,), (0,)), ((), ())), preferred_element_type=f32)


def halves(row):
    high = row.astype(bf16).astype(f32)
    return high, row - high


def rows16(*rows):
    n = rows[0].shape[1]
    at = lax.broadcasted_iota(jnp.int32, (16, n), 0)
    out = jnp.zeros((16, n), f32)
    for i, row in enumerate(rows):
        out = jnp.where(at == i, jnp.broadcast_to(row, (16, n)), out)
    return out.astype(bf16)


def turned(u, d):
    d = d % DK
    return u if d == 0 else pltpu.roll(u, DK - d, 0)


def features(u):
    n = u.shape[1]
    parts = [u, u * u * ROOT]
    for d in range(1, 8):
        parts.append(u * turned(u, d))
    parts.append(u[:8] * u[8:])
    first = lax.broadcasted_iota(jnp.int32, (8, n), 0) == 0
    parts.append(jnp.where(first, 1.0, 0.0).astype(f32))
    return jnp.concatenate(parts, 0).astype(bf16)


def pull_back(u, g):
    out = g[0:16] + (g[16:32] * (2.0 * ROOT)) * u
    for d in range(1, 8):
        pair = g[16 + 16 * d : 32 + 16 * d]
        out = out + pair * turned(u, d) + turned(pair * u, -d)
    pair = g[144:152]
    return out + jnp.concatenate([pair * u[8:], pair * u[:8]], 0)


def kernel(
    x_hbm, u_hbm, wq_hbm, wk_hbm, wv_hbm,
    gin, gwq, gwk, gwv,
    xb, ub, wq, wk, wv, xt2, xg,
    sqk, sv, rqk, rv, us, ur,
    fq, fk, vb, vt, ut, at, num, dloc, gnb, gdr, gfq, gfk, gvt, stb, nrm,
    st1, xr1, zs1, zr1, pb1, pf1,
    st2, xr2, zs2, zr2, pb2, pf2,
    gg, gb, gi, gacc, da, db, ra, rb, sa, fa, fb, fc, yb, yr, rs, rs_q, rs_k, rs_v, total,
    lsem, osem, ssem, rsem,
):
    z, x, y, c = (lax.axis_index(a) for a in SEQ_BATCH)
    place = {"seq_0": z, "seq_1": x, "seq_2": y}
    bytes_sent, groups = [0], [0]

    class Group:
        def __init__(self, like):
            self.like, self.k = like, groups[0]
            groups[0] += 1

        def copy(self, src, dst, target, k=0):
            return pltpu.make_async_remote_copy(
                src_ref=src, dst_ref=dst, send_sem=ssem.at[k], recv_sem=rsem.at[self.k],
                device_id=target, device_id_type=MESH_ID,
            )

        def send(self, src, dst, target, k=0):
            bytes_sent[0] += math.prod(src.shape) * 4 if k == 0 else 0
            self.copy(src, dst, target, k).start()

        def wait(self):
            self.copy(self.like, self.like, {"batch": 1 - c}).wait_recv()

    def one(src, dst, target):
        group = Group(dst)
        group.send(src, dst, target)
        return group

    def slot(place, j):
        return lax.rem(place - j + 7, N)

    def at_peer(axis, d):
        return lax.rem(place[axis] + d, N)

    loads = {}

    def load(name, k, src, dst):
        loads[name] = pltpu.make_async_copy(src, dst, lsem.at[k])
        loads[name].start()

    load("x", 0, x_hbm.at[0], xb)
    load("wq", 1, wq_hbm, wq)
    load("wk", 2, wk_hbm, wk)
    for k, dy in enumerate(ORDER):
        cols = pl.ds(pl.multiple_of(at_peer("seq_2", dy) * 256, 256), 256)
        load(("wv", k), 3 + k, wv_hbm.at[:, cols], wv.at[k])
    load("u", 7, u_hbm.at[0], ub)

    barrier = pltpu.get_barrier_semaphore()
    greeted = 0
    for d in range(N):
        for e in range(N):
            if d or e:
                greeted += 1
                pl.semaphore_signal(
                    barrier, inc=1, device_id_type=MESH_ID,
                    device_id={"seq_0": at_peer("seq_0", d), "seq_1": at_peer("seq_1", e)},
                )
        if d:
            greeted += 1
            pl.semaphore_signal(
                barrier, inc=1, device_id_type=MESH_ID, device_id={"seq_2": at_peer("seq_2", d)}
            )
        greeted += 1
        pl.semaphore_signal(
            barrier, inc=1, device_id_type=MESH_ID,
            device_id={"seq_2": at_peer("seq_2", d), "batch": 1 - c},
        )

    loads["x"].wait()
    loads["wq"].wait()
    qt = mm(xb[...], wq[...]).T
    loads["wk"].wait()
    kt = mm(xb[...], wk[...]).T
    for p in range(N):
        sqk[p, 0:32] = qt[32 * p : 32 * p + 32]
        sqk[p, 32:64] = kt[32 * p : 32 * p + 32]
    pl.semaphore_wait(barrier, greeted)
    qk_in = Group(rqk.at[pl.ds(0, 3)])
    for dy in (1, 3, 2):
        p = at_peer("seq_2", dy)
        qk_in.send(sqk.at[p], rqk.at[dy - 1], {"seq_2": p})
    rqk[3] = sqk[y]
    v_in = Group(rv.at[pl.ds(0, 3)])
    for k, dy in enumerate(ORDER):
        p = at_peer("seq_2", dy)
        loads[("wv", k)].wait()
        v = mm(xb[...], wv[k]).astype(bf16).astype(f32)
        if dy:
            sv[k] = v
            v_in.send(sv.at[k], rv.at[dy - 1], {"seq_2": p})
        else:
            rv[3] = v
    loads["u"].wait()
    for p in range(N):
        us[p] = ub[:, 256 * p : 256 * p + 256].astype(f32)
    u_in = Group(ur.at[pl.ds(0, 3)])
    for dy in (1, 3, 2):
        p = at_peer("seq_2", dy)
        u_in.send(us.at[p], ur.at[dy - 1], {"seq_2": p})
    ur[3] = us[y]

    for b in range(16):
        block = xb[:, 128 * b : 128 * b + 128].astype(f32).T
        for i in range(8):
            row = 64 * (b % 4) + 16 * (i // 2)
            xt2[i % 2, b // 4, row : row + 16] = block[16 * i : 16 * i + 16]
    chunk = [lax.rem(z + i + 1, N) for i in range(N)]
    after, before = at_peer("seq_2", 1), at_peer("seq_2", 3)
    x_in = [Group(xg.at[i, pl.ds(0, 5 if i < 3 else 4)]) for i in range(N)]
    passing = [None] * N

    def x_start(i):
        part = chunk[i]
        mine = xg.at[part, 2 * y + c]
        x_in[i].send(xt2.at[1 - c, part], mine, {"batch": 1 - c})
        up = one(xt2.at[c, part], mine, {"seq_2": after, "batch": c})
        x_in[i].send(xt2.at[c, part], mine, {"seq_2": before, "batch": c})
        x_in[i].send(xt2.at[1 - c, part], mine, {"seq_2": after, "batch": 1 - c})
        down = one(xt2.at[1 - c, part], mine, {"seq_2": before, "batch": 1 - c})
        xg[part, 2 * y + c] = xt2[c, part]
        passing[i] = (up, down)

    to_pair = one(xt2.at[1 - c, chunk[3]], xg.at[chunk[3], 2 * y + c], {"batch": 1 - c})
    xg[chunk[3], 2 * y + c] = xt2[c, chunk[3]]

    def x_start_last():
        part = chunk[3]
        mine = xg.at[part, 2 * y + c]
        up, down = Group(xg.at[3, 0]), Group(xg.at[3, 0])
        passing[3] = (up, down)
        up.send(xt2.at[c, part], mine, {"seq_2": after})
        x_in[3].send(xt2.at[c, part], mine, {"seq_2": before})
        to_pair.wait()

        @pl.when(c == 1)
        def _():
            for e in range(2):
                src = xg.at[part, 2 * y] if e else xt2.at[0, part]
                into = xg.at[part, 2 * y + 1 - e]
                x_in[3].send(src, into, {"seq_2": after, "batch": e}, 1)
                down.send(src, into, {"seq_2": before, "batch": e}, 1)

    def x_pass(i):
        part = chunk[i]
        up, down = passing[i]
        up.wait()
        move = xg.at[part, 2 * before + c]
        x_in[i].send(move, move, {"seq_2": after})
        down.wait()
        move = xg.at[part, 2 * after + 1 - c]
        x_in[i].send(move, move, {"seq_2": before})

    for i in range(N - 1):
        x_start(i)

    qk_in.wait()
    for h in range(2):
        lo = 16 * h
        uq = jnp.concatenate([rqk[slot(y, j), lo : lo + 16] for j in range(N)], 1) * 0.5
        uk = jnp.concatenate([rqk[slot(y, j), 32 + lo : 48 + lo] for j in range(N)], 1) * 0.5
        fq[h] = features(uq)
        fk[h] = features(uk)
    v_in.wait()
    ones = jnp.ones((16, TOK), bf16)
    for h in range(2):
        for j in range(N):
            vb[h, 128 * j : 128 * j + 128] = rv[slot(y, j), :, 128 * h : 128 * h + 128].astype(bf16)

    def put_state(st, h, state, norm):
        st[2 * h] = state[:80]
        st[2 * h + 1] = state[80:]
        st[2 * h + 1, 73:74] = norm[:, :128]
        st[2 * h + 1, 74:75] = jnp.concatenate([norm[:, 128:], jnp.zeros((1, 96), f32)], 1)

    def get_state(pf, h):
        low, high = slot(x, 2 * h), slot(x, 2 * h + 1)
        state = jnp.concatenate([pf[low], pf[high]], 0)
        norm = jnp.concatenate([pf[high, 73:74], pf[high, 74:75, :32]], 1)
        return state, norm

    for h in range(2):
        put_state(st1, h, mm(fk[h], vb[h]), mm_nt(ones, fk[h])[:1])

    def scan_start(st, xr):
        group = Group(xr.at[pl.ds(0, 3)])
        for d in (1, 3, 2):
            p = at_peer("seq_1", d)
            group.send(st.at[p], xr.at[d - 1], {"seq_1": p})
        xr[3] = st[x]
        return group

    def scan_mid(group, xr, zs, zr):
        group.wait()
        zs[...] = (xr[0] + xr[1]) + (xr[2] + xr[3])
        group = Group(zr)
        for d in (1, 3, 2):
            group.send(zs, zr.at[d - 1], {"seq_0": at_peer("seq_0", d)})
        return group

    def scan_back(group, xr, zr, pb, pf, later):
        group.wait()
        run = jnp.zeros((80, 128), f32)
        for d in (1, 2, 3):
            run = run + jnp.where(z < d if later else z >= d, zr[d - 1], 0.0)
        for i in reversed(range(N)) if later else range(N):
            pb[i] = run
            run = run + xr[slot(x, i)]
        group = Group(pf.at[pl.ds(0, 3)])
        for d in (1, 3, 2):
            p = at_peer("seq_1", d)
            group.send(pb.at[p], pf.at[d - 1], {"seq_1": p})
        pf[3] = pb[x]
        return group

    keep = lax.broadcasted_iota(jnp.int32, (TOK, TOK), 1) >= lax.broadcasted_iota(
        jnp.int32, (TOK, TOK), 0
    )

    def local_forward(h):
        for j in range(N):
            vt[h, :, 128 * j : 128 * j + 128] = (
                rv[slot(y, j), :, 128 * h : 128 * h + 128].T.astype(bf16)
            )
        scores = jnp.where(keep, mm_tn(fk[h], fq[h]), 0.0)
        dloc[h] = jnp.broadcast_to(jnp.sum(scores, 0, keepdims=True), (8, TOK))
        at[h] = scores.astype(bf16)
        num[h] = mm(vt[h], at[h])

    move = scan_start(st1, xr1)
    local_forward(0)
    move = scan_mid(move, xr1, zs1, zr1)
    local_forward(1)
    move = scan_back(move, xr1, zr1, pb1, pf1, False)
    u_in.wait()
    for h in range(2):
        for j in range(N):
            ut[h, :, 128 * j : 128 * j + 128] = ur[slot(y, j), :, 128 * h : 128 * h + 128].T
    move.wait()

    for h in range(2):
        state, norm = get_state(pf1, h)
        stb[h] = state.astype(bf16)
        n_hi, n_lo = halves(norm)
        nrm[h] = jnp.concatenate([n_hi, n_lo, n_hi, jnp.zeros((5, FP), f32)], 0)
        numer = num[h] + mm_tn(stb[h], fq[h])
        denom = dloc[h, :1] + jnp.sum(mm(rows16(n_hi, n_lo), fq[h]), 0, keepdims=True)
        inverse = 1.0 / denom
        upstream = ut[h]
        g_num = upstream * inverse
        g_den = -jnp.sum(upstream * (numer * inverse), 0, keepdims=True) * inverse
        gnb[h] = g_num.astype(bf16)
        g_hi, g_lo = halves(g_den)
        gdr[h] = jnp.concatenate([g_hi, g_lo, jnp.zeros((6, TOK), f32)], 0)
        back = mm_nt(fq[h], gnb[h])
        back_norm = jnp.sum(mm_nt(rows16(g_hi, g_lo), fq[h]), 0, keepdims=True)
        put_state(st2, h, back, back_norm)

    def local_backward(h):
        g_hi, g_lo = gdr[h, 0:1], gdr[h, 1:2]
        n_hi, n_lo = nrm[h, 0:1], nrm[h, 1:2]
        inner = mm(vb[h], gnb[h]) + (g_hi + g_lo)
        ga = jnp.where(keep, inner, 0.0).astype(bf16)
        outer = mm_tn(rows16(n_hi, n_lo, n_hi), rows16(g_hi, g_hi, g_lo))
        gfq[h] = mm(fk[h], ga) + mm(stb[h], gnb[h]) + outer
        gvt[h] = mm_nt(gnb[h], at[h])
        gfk[h] = mm_nt(fq[h], ga)

    def put_grad(h, first, u, grad):
        out = (pull_back(u, grad) * 0.5).astype(bf16).astype(f32)
        for j in range(N):
            gg[c, j, first + 16 * h : first + 16 * h + 16] = out[:, 128 * j : 128 * j + 128]

    move = scan_start(st2, xr2)
    x_pass(0)
    x_start_last()
    local_backward(0)
    move = scan_mid(move, xr2, zs2, zr2)
    x_pass(1)
    local_backward(1)
    move = scan_back(move, xr2, zr2, pb2, pf2, True)
    for h in range(2):
        lo = 16 * h
        uq = jnp.concatenate([rqk[slot(y, j), lo : lo + 16] for j in range(N)], 1) * 0.5
        put_grad(h, 256, uq, gfq[h])
    move.wait()
    first16 = lax.broadcasted_iota(jnp.int32, (16, TOK), 0) < 2
    flag = jnp.where(first16, 1.0, 0.0).astype(bf16)
    for h in range(2):
        back, back_norm = get_state(pf2, h)
        backb = back.astype(bf16)
        b_hi, b_lo = halves(back_norm)
        g_val = gvt[h] + mm_tn(backb, fk[h])
        g_val = g_val.astype(bf16).astype(f32)
        for j in range(N):
            gg[c, j, 128 * h : 128 * h + 128] = g_val[:, 128 * j : 128 * j + 128]
        g_fk = gfk[h] + mm(backb, vt[h]) + mm_tn(rows16(b_hi, b_lo), flag)
        lo = 32 + 16 * h
        uk = jnp.concatenate([rqk[slot(y, j), lo : lo + 16] for j in range(N)], 1) * 0.5
        put_grad(h, 288, uk, g_fk)

    pair_g = one(gg.at[c], gg.at[c], {"batch": 1 - c})
    x_pass(2)
    gb[3] = gg[c, y]
    gacc[...] = mm(wv[3], gb[3, 0:256].astype(bf16))
    x_pass(3)
    pair_g.wait()
    rhs = jnp.concatenate([gg[i, j].astype(bf16) for j in range(N) for i in range(2)], 1)

    a_in = [Group(ra.at[i]) for i in range(N)]
    b_in, c_last = Group(rb), Group(fc)

    def weights_of(i):
        part = chunk[i]
        lhs = jnp.concatenate(
            [xg[part, j].astype(bf16) for j in range(8)], 1
        )
        out = mm_nt(lhs, rhs)
        for xx in range(N):
            for j in range(N):
                own = out[64 * xx + 16 * j : 64 * xx + 16 * j + 16]
                thin = own[:, 256:320]
                da[i, xx, 24 * j : 24 * j + 16] = own[:, :128]
                da[i, xx, 24 * j + 16 : 24 * j + 24] = jnp.concatenate([thin[:8], thin[8:]], 1)
                db[i, xx, 16 * j : 16 * j + 16] = own[:, 128:256]
        for k, d in enumerate((1, 3, 2)):
            p = at_peer("seq_1", d)
            a_in[i].send(da.at[i, p], ra.at[i, k], {"seq_1": p})
        if i < 2:
            b_in.send(db.at[i], rb.at[i], {"seq_0": part})
        elif i == 2:
            for d in (1, 3, 2, 0):
                p = at_peer("seq_1", d)
                c_last.send(db.at[i, p], fc.at[(d + 3) % 4], {"seq_0": part, "seq_1": p})

    a_last, b_last = Group(fa), Group(fb)

    def a_onward(i):
        a_in[i].wait()
        sa[i] = (da[i, x] + ra[i, 0]) + (ra[i, 1] + ra[i, 2])
        if i < N - 1:
            a_last.send(sa.at[i], fa.at[i], {"seq_0": chunk[i]})

    x_in[0].wait()
    weights_of(0)
    x_in[1].wait()
    weights_of(1)
    x_in[2].wait()
    weights_of(2)
    g_thin = Group(gb.at[pl.ds(0, 3), pl.ds(256, 64)])
    a_onward(0)
    x_in[3].wait()
    g_wide = {}
    for dy in (2, 1, 3):
        p = at_peer("seq_2", dy)
        g_thin.send(gg.at[c, p, pl.ds(256, 64)], gb.at[dy - 1, pl.ds(256, 64)], {"seq_2": p})
    for dy in (2, 1, 3):
        p = at_peer("seq_2", dy)
        g_wide[dy] = one(gg.at[c, p, pl.ds(0, 256)], gb.at[dy - 1, pl.ds(0, 256)], {"seq_2": p})
    weights_of(3)
    b_in.wait()
    for xx in range(N):
        db[3, xx] = db[3, xx] + (rb[0, xx] + rb[1, xx])
    for d in (1, 3, 2):
        p = at_peer("seq_1", d)
        b_last.send(db.at[3, p], fb.at[d - 1], {"seq_1": p})
    a_onward(1)
    a_onward(2)

    a_onward(3)
    a_last.wait()
    b_last.wait()
    c_last.wait()
    sum_a = (sa[3] + fa[0]) + (fa[1] + fa[2])
    sum_b = (db[3, x] + fb[0]) + (fb[1] + fb[2])
    sum_b = sum_b + ((fc[0] + fc[1]) + (fc[2] + fc[3]))
    for j in range(N):
        yb[j, 0:24] = sum_a[24 * j : 24 * j + 24]
        yb[j, 24:40] = sum_b[16 * j : 16 * j + 16]
    y_in = Group(yr.at[pl.ds(0, 3)])
    for dy in (2, 1, 3):
        p = at_peer("seq_2", dy)
        y_in.send(yb.at[p], yr.at[dy - 1], {"seq_2": p})
    yr[3] = yb[y]
    g_thin.wait()
    g_wide[2].wait()
    rows = [gb[slot(y, j), 256:288] for j in range(N)] + [gb[slot(y, j), 288:320] for j in range(N)]
    part = jnp.concatenate(rows + [gb[1, 0:256]], 0).astype(bf16)
    gacc[...] = gacc[...] + mm(jnp.concatenate([wq[...], wk[...], wv[2]], 1), part)
    g_wide[1].wait()
    g_wide[3].wait()
    part = jnp.concatenate([gb[2, 0:256], gb[0, 0:256]], 0).astype(bf16)
    gacc[...] = gacc[...] + mm(jnp.concatenate([wv[0], wv[1]], 1), part)
    for i in range(16):
        gi[:, 128 * i : 128 * i + 128] = gacc[128 * i : 128 * i + 128].T.astype(bf16)
    out_copy = pltpu.make_async_copy(gi, gin.at[0], osem.at[0])
    out_copy.start()
    y_in.wait()
    for dy in range(N):
        rs[at_peer("seq_2", (4 - dy) % 4)] = yr[(dy + 3) % 4]
    lane = lax.broadcasted_iota(jnp.int32, (16, 128), 1) // 32
    w_q = jnp.zeros((16, 128), f32)
    w_k = jnp.zeros((16, 128), f32)
    for p in range(N):
        rs_v[:, 256 * p : 256 * p + 128] = rs[p, 0:16]
        rs_v[:, 256 * p + 128 : 256 * p + 256] = rs[p, 24:40]
        thin = rs[p, 16:24]
        thin = jnp.concatenate([thin, pltpu.roll(thin, 64, 1)], 0)
        from_q = pltpu.roll(thin, 32 * p, 1) if p else thin
        w_q = jnp.where(lane == p, from_q, w_q)
        from_k = pltpu.roll(thin, (32 * p + 96) % 128, 1) if p != 1 else thin
        w_k = jnp.where(lane == p, from_k, w_k)
    rs_q[...] = w_q
    rs_k[...] = w_k
    results = [out_copy]
    for i, (src, dst) in enumerate(((rs_q, gwq), (rs_k, gwk), (rs_v, gwv))):
        results.append(pltpu.make_async_copy(src, dst, osem.at[i + 1]))
        results[-1].start()
    for copy in results:
        copy.wait()
    assert groups[0] == GROUPS and bytes_sent[0] == SENT * 512
    to_pair.copy(total, total, {"batch": 1 - c}).wait_send()

    @pl.when(c == 1)
    def _():
        many = total.at[pl.ds(0, 4 * 256)]
        to_pair.copy(many, many, {"batch": 1 - c}, 1).wait_send()


def finish(*refs):
    sources, results, sems = refs[:4], refs[4:8], refs[8]
    copies = [
        pltpu.make_async_copy(src, dst, sems.at[i])
        for i, (src, dst) in enumerate(zip(sources, results))
    ]
    for copy in copies:
        copy.start()
    for copy in copies:
        copy.wait()


GROUPS = 3 + 6 + 4 * 3 + 1 + 1 + 4 + 4 + 1 + 4
SENT = (
    3 * 64 + 6 * 256 + 18 * 80 + 26 * 256 + 4 * 320 + 3 * 320
    + 12 * 96 + 12 * 64 + 3 * 96 + 3 * 64 + 3 * 40
)


def body(inputs, cotangent, w_query, w_key, w_value):
    vmem = pltpu.VMEM
    hbm = pl.BlockSpec(memory_space=pl.ANY)
    scan = [
        vmem((4, 80, 128), f32), vmem((4, 80, 128), f32), vmem((80, 128), f32),
        vmem((3, 80, 128), f32), vmem((4, 80, 128), f32), vmem((4, 80, 128), f32),
    ]
    scratch = [
        vmem((BLK, D), bf16), vmem((BLK, 1024), bf16), vmem((D, 128), bf16), vmem((D, 128), bf16),
        vmem((4, D, 256), bf16), vmem((2, 4, 256, 128), f32), vmem((4, 8, 256, 128), f32),
        vmem((4, 64, 128), f32), vmem((3, 128, 256), f32), vmem((4, 64, 128), f32),
        vmem((4, 128, 256), f32), vmem((4, 128, 256), f32), vmem((4, 128, 256), f32),
        vmem((2, FP, TOK), bf16), vmem((2, FP, TOK), bf16), vmem((2, TOK, 128), bf16),
        vmem((2, 128, TOK), bf16), vmem((2, 128, TOK), f32), vmem((2, TOK, TOK), bf16),
        vmem((2, 128, TOK), f32), vmem((2, 8, TOK), f32), vmem((2, 128, TOK), bf16),
        vmem((2, 8, TOK), f32), vmem((2, FP, TOK), f32), vmem((2, FP, TOK), f32),
        vmem((2, 128, TOK), f32), vmem((2, FP, 128), bf16), vmem((2, 8, FP), f32),
        *scan, *scan,
        vmem((2, 4, 320, 128), f32), vmem((4, 320, 128), f32), vmem((BLK, D), bf16),
        vmem((D, BLK), f32), vmem((4, 4, 96, 128), f32), vmem((4, 4, 64, 128), f32),
        vmem((4, 3, 96, 128), f32), vmem((2, 4, 64, 128), f32),
        vmem((4, 96, 128), f32), vmem((3, 96, 128), f32), vmem((3, 64, 128), f32),
        vmem((4, 64, 128), f32),
        vmem((4, 40, 128), f32), vmem((4, 40, 128), f32),
        vmem((4, 40, 128), f32), vmem((16, 128), f32), vmem((16, 128), f32),
        vmem((16, 1024), f32), vmem((SENT, 128), f32),
        pltpu.SemaphoreType.DMA((8,)), pltpu.SemaphoreType.DMA((4,)), pltpu.SemaphoreType.DMA((2,)),
        pltpu.SemaphoreType.DMA((GROUPS,)),
    ]
    shapes = (((1, BLK, D), bf16), ((16, 128), f32), ((16, 128), f32), ((16, 1024), f32))
    results = pl.pallas_call(
        kernel,
        out_shape=tuple(pltpu.VMEM(*shape) for shape in shapes),
        in_specs=[pl.BlockSpec(memory_space=pltpu.HBM)] * 5,
        out_specs=(hbm,) * 4,
        scratch_shapes=scratch,
        compiler_params=pltpu.CompilerParams(
            collective_id=0, has_side_effects=True, vmem_limit_bytes=60 * 1024 * 1024
        ),
    )(inputs, cotangent, w_query, w_key, w_value)
    return pl.pallas_call(
        finish,
        out_shape=tuple(jax.ShapeDtypeStruct(*shape) for shape in shapes),
        in_specs=[hbm] * 4,
        out_specs=(pl.BlockSpec(memory_space=pltpu.HBM),) * 4,
        scratch_shapes=[pltpu.SemaphoreType.DMA((4,))],
        compiler_params=pltpu.CompilerParams(vmem_limit_bytes=4 * 1024 * 1024),
    )(*results)


def solution(mesh):
    split = Mesh(
        mesh.devices.reshape(4, 4, 4, mesh.shape["batch"]), ("seq_0", "seq_1", "seq_2", "batch")
    )
    in_specs = (P("batch", SEQ, None), P("batch", SEQ, None), P(), P(), P())
    out_specs = (P("batch", SEQ, None), P(SEQ_BATCH, None), P(SEQ_BATCH, None), P(SEQ_BATCH, None))
    return jax.shard_map(body, mesh=split, in_specs=in_specs, out_specs=out_specs, check_vma=False)
```

```python
import math

import jax
import jax.numpy as jnp
from jax import lax
from jax.experimental import pallas as pl
from jax.experimental.pallas import tpu as pltpu
from jax.sharding import Mesh
from jax.sharding import PartitionSpec as P

D = 2048
H = 8
DK = 16
DV = 128
SEQ = ("seq_0", "seq_1", "seq_2")
SEQ_BATCH = ("seq_0", "seq_1", "seq_2", "batch")
N = 4
BLK = 128
TOK = N * BLK
FP = 160
ROOT = 1.0 / math.sqrt(2.0)
ORDER = (1, 3, 2, 0)
f32 = jnp.float32
bf16 = jnp.bfloat16
MESH_ID = pl.DeviceIdType.MESH


def mm(a, b):
    return lax.dot_general(a, b, (((1,), (0,)), ((), ())), preferred_element_type=f32)


def mm_nt(a, b):
    return lax.dot_general(a, b, (((1,), (1,)), ((), ())), preferred_element_type=f32)


def mm_tn(a, b):
    return lax.dot_general(a, b, (((0,), (0,)), ((), ())), preferred_element_type=f32)


def halves(row):
    high = row.astype(bf16).astype(f32)
    return high, row - high


def rows16(*rows):
    n = rows[0].shape[1]
    at = lax.broadcasted_iota(jnp.int32, (16, n), 0)
    out = jnp.zeros((16, n), f32)
    for i, row in enumerate(rows):
        out = jnp.where(at == i, jnp.broadcast_to(row, (16, n)), out)
    return out.astype(bf16)


def turned(u, d):
    d = d % DK
    return u if d == 0 else pltpu.roll(u, DK - d, 0)


def features(u):
    n = u.shape[1]
    parts = [u, u * u * ROOT]
    for d in range(1, 8):
        parts.append(u * turned(u, d))
    parts.append(u[:8] * u[8:])
    first = lax.broadcasted_iota(jnp.int32, (8, n), 0) == 0
    parts.append(jnp.where(first, 1.0, 0.0).astype(f32))
    return jnp.concatenate(parts, 0).astype(bf16)


def pull_back(u, g):
    out = g[0:16] + (g[16:32] * (2.0 * ROOT)) * u
    for d in range(1, 8):
        pair = g[16 + 16 * d : 32 + 16 * d]
        out = out + pair * turned(u, d) + turned(pair * u, -d)
    pair = g[144:152]
    return out + jnp.concatenate([pair * u[8:], pair * u[:8]], 0)


def kernel(
    x_hbm, u_hbm, wq_hbm, wk_hbm, wv_hbm,
    gin, gwq, gwk, gwv,
    xb, ub, wq, wk, wv, xt2, xg,
    sqk, sv, rqk, rv, us, ur,
    fq, fk, vb, vt, ut, at, num, dloc, gnb, gdr, gfq, gfk, gvt, stb, nrm,
    st1, xr1, zs1, zr1, pb1, pf1,
    st2, xr2, zs2, zr2, pb2, pf2,
    gg, gb, gi, gacc, da, db, ra, rb, sa, fa, fb, fc, yb, yr, rs, rs_q, rs_k, rs_v, total,
    lsem, osem, ssem, rsem,
):
    z, x, y, c = (lax.axis_index(a) for a in SEQ_BATCH)
    place = {"seq_0": z, "seq_1": x, "seq_2": y}
    bytes_sent, groups = [0], [0]

    class Group:
        def __init__(self, like):
            self.like, self.k = like, groups[0]
            groups[0] += 1

        def copy(self, src, dst, target, k=0):
            return pltpu.make_async_remote_copy(
                src_ref=src, dst_ref=dst, send_sem=ssem.at[k], recv_sem=rsem.at[self.k],
                device_id=target, device_id_type=MESH_ID,
            )

        def send(self, src, dst, target, k=0):
            bytes_sent[0] += math.prod(src.shape) * 4 if k == 0 else 0
            self.copy(src, dst, target, k).start()

        def wait(self):
            self.copy(self.like, self.like, {"batch": 1 - c}).wait_recv()

    def one(src, dst, target):
        group = Group(dst)
        group.send(src, dst, target)
        return group

    def slot(place, j):
        return lax.rem(place - j + 7, N)

    def at_peer(axis, d):
        return lax.rem(place[axis] + d, N)

    loads = {}

    def load(name, k, src, dst):
        loads[name] = pltpu.make_async_copy(src, dst, lsem.at[k])
        loads[name].start()

    load("x", 0, x_hbm.at[0], xb)
    load("wq", 1, wq_hbm, wq)
    load("wk", 2, wk_hbm, wk)
    for k, dy in enumerate(ORDER):
        cols = pl.ds(pl.multiple_of(at_peer("seq_2", dy) * 256, 256), 256)
        load(("wv", k), 3 + k, wv_hbm.at[:, cols], wv.at[k])
    load("u", 7, u_hbm.at[0], ub)

    barrier = pltpu.get_barrier_semaphore()
    greeted = 0
    for d in range(N):
        for e in range(N):
            if d or e:
                greeted += 1
                pl.semaphore_signal(
                    barrier, inc=1, device_id_type=MESH_ID,
                    device_id={"seq_0": at_peer("seq_0", d), "seq_1": at_peer("seq_1", e)},
                )
        if d:
            greeted += 1
            pl.semaphore_signal(
                barrier, inc=1, device_id_type=MESH_ID, device_id={"seq_2": at_peer("seq_2", d)}
            )
        greeted += 1
        pl.semaphore_signal(
            barrier, inc=1, device_id_type=MESH_ID,
            device_id={"seq_2": at_peer("seq_2", d), "batch": 1 - c},
        )

    loads["x"].wait()
    loads["wq"].wait()
    qt = mm(xb[...], wq[...]).T
    loads["wk"].wait()
    kt = mm(xb[...], wk[...]).T
    for p in range(N):
        sqk[p, 0:32] = qt[32 * p : 32 * p + 32]
        sqk[p, 32:64] = kt[32 * p : 32 * p + 32]
    pl.semaphore_wait(barrier, greeted)
    qk_in = Group(rqk.at[pl.ds(0, 3)])
    for dy in (1, 3, 2):
        p = at_peer("seq_2", dy)
        qk_in.send(sqk.at[p], rqk.at[dy - 1], {"seq_2": p})
    rqk[3] = sqk[y]
    v_in = Group(rv.at[pl.ds(0, 3)])
    for k, dy in enumerate(ORDER):
        p = at_peer("seq_2", dy)
        loads[("wv", k)].wait()
        v = mm(xb[...], wv[k]).astype(bf16).astype(f32)
        if dy:
            sv[k] = v
            v_in.send(sv.at[k], rv.at[dy - 1], {"seq_2": p})
        else:
            rv[3] = v
    loads["u"].wait()
    for p in range(N):
        us[p] = ub[:, 256 * p : 256 * p + 256].astype(f32)
    u_in = Group(ur.at[pl.ds(0, 3)])
    for dy in (1, 3, 2):
        p = at_peer("seq_2", dy)
        u_in.send(us.at[p], ur.at[dy - 1], {"seq_2": p})
    ur[3] = us[y]

    for b in range(16):
        block = xb[:, 128 * b : 128 * b + 128].astype(f32).T
        for i in range(8):
            row = 64 * (b % 4) + 16 * (i // 2)
            xt2[i % 2, b // 4, row : row + 16] = block[16 * i : 16 * i + 16]
    chunk = [lax.rem(z + i + 1, N) for i in range(N)]
    after, before = at_peer("seq_2", 1), at_peer("seq_2", 3)
    x_in = [Group(xg.at[i, pl.ds(0, 5 if i < 3 else 4)]) for i in range(N)]
    passing = [None] * N

    def x_start(i):
        part = chunk[i]
        mine = xg.at[part, 2 * y + c]
        x_in[i].send(xt2.at[1 - c, part], mine, {"batch": 1 - c})
        up = one(xt2.at[c, part], mine, {"seq_2": after, "batch": c})
        x_in[i].send(xt2.at[c, part], mine, {"seq_2": before, "batch": c})
        x_in[i].send(xt2.at[1 - c, part], mine, {"seq_2": after, "batch": 1 - c})
        down = one(xt2.at[1 - c, part], mine, {"seq_2": before, "batch": 1 - c})
        xg[part, 2 * y + c] = xt2[c, part]
        passing[i] = (up, down)

    to_pair = one(xt2.at[1 - c, chunk[3]], xg.at[chunk[3], 2 * y + c], {"batch": 1 - c})
    xg[chunk[3], 2 * y + c] = xt2[c, chunk[3]]

    def x_start_last():
        part = chunk[3]
        mine = xg.at[part, 2 * y + c]
        up, down = Group(xg.at[3, 0]), Group(xg.at[3, 0])
        passing[3] = (up, down)
        up.send(xt2.at[c, part], mine, {"seq_2": after})
        x_in[3].send(xt2.at[c, part], mine, {"seq_2": before})
        to_pair.wait()

        @pl.when(c == 1)
        def _():
            for e in range(2):
                src = xg.at[part, 2 * y] if e else xt2.at[0, part]
                into = xg.at[part, 2 * y + 1 - e]
                x_in[3].send(src, into, {"seq_2": after, "batch": e}, 1)
                down.send(src, into, {"seq_2": before, "batch": e}, 1)

    def x_pass(i):
        part = chunk[i]
        up, down = passing[i]
        up.wait()
        move = xg.at[part, 2 * before + c]
        x_in[i].send(move, move, {"seq_2": after})
        down.wait()
        move = xg.at[part, 2 * after + 1 - c]
        x_in[i].send(move, move, {"seq_2": before})

    for i in range(N - 1):
        x_start(i)

    qk_in.wait()
    for h in range(2):
        lo = 16 * h
        uq = jnp.concatenate([rqk[slot(y, j), lo : lo + 16] for j in range(N)], 1) * 0.5
        uk = jnp.concatenate([rqk[slot(y, j), 32 + lo : 48 + lo] for j in range(N)], 1) * 0.5
        fq[h] = features(uq)
        fk[h] = features(uk)
    v_in.wait()
    ones = jnp.ones((16, TOK), bf16)
    for h in range(2):
        for j in range(N):
            vb[h, 128 * j : 128 * j + 128] = rv[slot(y, j), :, 128 * h : 128 * h + 128].astype(bf16)

    def put_state(st, h, state, norm):
        st[2 * h] = state[:80]
        st[2 * h + 1] = state[80:]
        st[2 * h + 1, 73:74] = norm[:, :128]
        st[2 * h + 1, 74:75] = jnp.concatenate([norm[:, 128:], jnp.zeros((1, 96), f32)], 1)

    def get_state(pf, h):
        low, high = slot(x, 2 * h), slot(x, 2 * h + 1)
        state = jnp.concatenate([pf[low], pf[high]], 0)
        norm = jnp.concatenate([pf[high, 73:74], pf[high, 74:75, :32]], 1)
        return state, norm

    for h in range(2):
        put_state(st1, h, mm(fk[h], vb[h]), mm_nt(ones, fk[h])[:1])

    def scan_start(st, xr):
        group = Group(xr.at[pl.ds(0, 3)])
        for d in (1, 3, 2):
            p = at_peer("seq_1", d)
            group.send(st.at[p], xr.at[d - 1], {"seq_1": p})
        xr[3] = st[x]
        return group

    def scan_mid(group, xr, zs, zr):
        group.wait()
        zs[...] = (xr[0] + xr[1]) + (xr[2] + xr[3])
        group = Group(zr)
        for d in (1, 3, 2):
            group.send(zs, zr.at[d - 1], {"seq_0": at_peer("seq_0", d)})
        return group

    def scan_back(group, xr, zr, pb, pf, later):
        group.wait()
        run = jnp.zeros((80, 128), f32)
        for d in (1, 2, 3):
            run = run + jnp.where(z < d if later else z >= d, zr[d - 1], 0.0)
        for i in reversed(range(N)) if later else range(N):
            pb[i] = run
            run = run + xr[slot(x, i)]
        group = Group(pf.at[pl.ds(0, 3)])
        for d in (1, 3, 2):
            p = at_peer("seq_1", d)
            group.send(pb.at[p], pf.at[d - 1], {"seq_1": p})
        pf[3] = pb[x]
        return group

    keep = lax.broadcasted_iota(jnp.int32, (TOK, TOK), 1) >= lax.broadcasted_iota(
        jnp.int32, (TOK, TOK), 0
    )

    def local_forward(h):
        for j in range(N):
            vt[h, :, 128 * j : 128 * j + 128] = (
                rv[slot(y, j), :, 128 * h : 128 * h + 128].T.astype(bf16)
            )
        scores = jnp.where(keep, mm_tn(fk[h], fq[h]), 0.0)
        dloc[h] = jnp.broadcast_to(jnp.sum(scores, 0, keepdims=True), (8, TOK))
        at[h] = scores.astype(bf16)
        num[h] = mm(vt[h], at[h])

    move = scan_start(st1, xr1)
    local_forward(0)
    move = scan_mid(move, xr1, zs1, zr1)
    local_forward(1)
    move = scan_back(move, xr1, zr1, pb1, pf1, False)
    u_in.wait()
    for h in range(2):
        for j in range(N):
            ut[h, :, 128 * j : 128 * j + 128] = ur[slot(y, j), :, 128 * h : 128 * h + 128].T
    move.wait()

    for h in range(2):
        state, norm = get_state(pf1, h)
        stb[h] = state.astype(bf16)
        n_hi, n_lo = halves(norm)
        nrm[h] = jnp.concatenate([n_hi, n_lo, n_hi, jnp.zeros((5, FP), f32)], 0)
        numer = num[h] + mm_tn(stb[h], fq[h])
        denom = dloc[h, :1] + jnp.sum(mm(rows16(n_hi, n_lo), fq[h]), 0, keepdims=True)
        inverse = 1.0 / denom
        upstream = ut[h]
        g_num = upstream * inverse
        g_den = -jnp.sum(upstream * (numer * inverse), 0, keepdims=True) * inverse
        gnb[h] = g_num.astype(bf16)
        g_hi, g_lo = halves(g_den)
        gdr[h] = jnp.concatenate([g_hi, g_lo, jnp.zeros((6, TOK), f32)], 0)
        back = mm_nt(fq[h], gnb[h])
        back_norm = jnp.sum(mm_nt(rows16(g_hi, g_lo), fq[h]), 0, keepdims=True)
        put_state(st2, h, back, back_norm)

    def local_backward(h):
        g_hi, g_lo = gdr[h, 0:1], gdr[h, 1:2]
        n_hi, n_lo = nrm[h, 0:1], nrm[h, 1:2]
        inner = mm(vb[h], gnb[h]) + (g_hi + g_lo)
        ga = jnp.where(keep, inner, 0.0).astype(bf16)
        outer = mm_tn(rows16(n_hi, n_lo, n_hi), rows16(g_hi, g_hi, g_lo))
        gfq[h] = mm(fk[h], ga) + mm(stb[h], gnb[h]) + outer
        gvt[h] = mm_nt(gnb[h], at[h])
        gfk[h] = mm_nt(fq[h], ga)

    def put_grad(h, first, u, grad):
        out = (pull_back(u, grad) * 0.5).astype(bf16).astype(f32)
        for j in range(N):
            gg[c, j, first + 16 * h : first + 16 * h + 16] = out[:, 128 * j : 128 * j + 128]

    move = scan_start(st2, xr2)
    x_pass(0)
    x_start_last()
    local_backward(0)
    move = scan_mid(move, xr2, zs2, zr2)
    x_pass(1)
    local_backward(1)
    move = scan_back(move, xr2, zr2, pb2, pf2, True)
    x_pass(2)
    for h in range(2):
        lo = 16 * h
        uq = jnp.concatenate([rqk[slot(y, j), lo : lo + 16] for j in range(N)], 1) * 0.5
        put_grad(h, 256, uq, gfq[h])
    move.wait()
    first16 = lax.broadcasted_iota(jnp.int32, (16, TOK), 0) < 2
    flag = jnp.where(first16, 1.0, 0.0).astype(bf16)
    for h in range(2):
        back, back_norm = get_state(pf2, h)
        backb = back.astype(bf16)
        b_hi, b_lo = halves(back_norm)
        g_val = gvt[h] + mm_tn(backb, fk[h])
        g_val = g_val.astype(bf16).astype(f32)
        for j in range(N):
            gg[c, j, 128 * h : 128 * h + 128] = g_val[:, 128 * j : 128 * j + 128]
        g_fk = gfk[h] + mm(backb, vt[h]) + mm_tn(rows16(b_hi, b_lo), flag)
        lo = 32 + 16 * h
        uk = jnp.concatenate([rqk[slot(y, j), lo : lo + 16] for j in range(N)], 1) * 0.5
        put_grad(h, 288, uk, g_fk)

    pair_g = one(gg.at[c], gg.at[c], {"batch": 1 - c})
    gb[3] = gg[c, y]
    gacc[...] = mm(wv[3], gb[3, 0:256].astype(bf16))
    pair_g.wait()
    rhs = jnp.concatenate([gg[i, j].astype(bf16) for j in range(N) for i in range(2)], 1)

    a_in = [Group(ra.at[i]) for i in range(N)]
    b_in, c_last = Group(rb), Group(fc)

    def weights_of(i):
        part = chunk[i]
        lhs = jnp.concatenate(
            [xg[part, j].astype(bf16) for j in range(8)], 1
        )
        out = mm_nt(lhs, rhs)
        for xx in range(N):
            for j in range(N):
                own = out[64 * xx + 16 * j : 64 * xx + 16 * j + 16]
                thin = own[:, 256:320]
                da[i, xx, 24 * j : 24 * j + 16] = own[:, :128]
                da[i, xx, 24 * j + 16 : 24 * j + 24] = jnp.concatenate([thin[:8], thin[8:]], 1)
                db[i, xx, 16 * j : 16 * j + 16] = own[:, 128:256]
        for k, d in enumerate((1, 3, 2)):
            p = at_peer("seq_1", d)
            a_in[i].send(da.at[i, p], ra.at[i, k], {"seq_1": p})
        if i < 2:
            b_in.send(db.at[i], rb.at[i], {"seq_0": part})
        elif i == 2:
            for d in (1, 3, 2, 0):
                p = at_peer("seq_1", d)
                c_last.send(db.at[i, p], fc.at[(d + 3) % 4], {"seq_0": part, "seq_1": p})

    a_last, b_last = Group(fa), Group(fb)

    def a_onward(i):
        a_in[i].wait()
        sa[i] = (da[i, x] + ra[i, 0]) + (ra[i, 1] + ra[i, 2])
        if i < N - 1:
            a_last.send(sa.at[i], fa.at[i], {"seq_0": chunk[i]})

    x_in[0].wait()
    weights_of(0)
    x_pass(3)
    x_in[1].wait()
    weights_of(1)
    x_in[2].wait()
    weights_of(2)
    g_thin = Group(gb.at[pl.ds(0, 3), pl.ds(256, 64)])
    a_onward(0)
    x_in[3].wait()
    g_wide = {}
    for dy in (2, 1, 3):
        p = at_peer("seq_2", dy)
        g_thin.send(gg.at[c, p, pl.ds(256, 64)], gb.at[dy - 1, pl.ds(256, 64)], {"seq_2": p})
    for dy in (2, 1, 3):
        p = at_peer("seq_2", dy)
        g_wide[dy] = one(gg.at[c, p, pl.ds(0, 256)], gb.at[dy - 1, pl.ds(0, 256)], {"seq_2": p})
    weights_of(3)
    b_in.wait()
    for xx in range(N):
        db[3, xx] = db[3, xx] + (rb[0, xx] + rb[1, xx])
    for d in (1, 3, 2):
        p = at_peer("seq_1", d)
        b_last.send(db.at[3, p], fb.at[d - 1], {"seq_1": p})
    a_onward(1)
    a_onward(2)

    a_onward(3)
    a_last.wait()
    b_last.wait()
    c_last.wait()
    sum_a = (sa[3] + fa[0]) + (fa[1] + fa[2])
    sum_b = (db[3, x] + fb[0]) + (fb[1] + fb[2])
    sum_b = sum_b + ((fc[0] + fc[1]) + (fc[2] + fc[3]))
    for j in range(N):
        yb[j, 0:24] = sum_a[24 * j : 24 * j + 24]
        yb[j, 24:40] = sum_b[16 * j : 16 * j + 16]
    y_in = Group(yr.at[pl.ds(0, 3)])
    for dy in (2, 1, 3):
        p = at_peer("seq_2", dy)
        y_in.send(yb.at[p], yr.at[dy - 1], {"seq_2": p})
    yr[3] = yb[y]
    g_thin.wait()
    g_wide[2].wait()
    rows = [gb[slot(y, j), 256:288] for j in range(N)] + [gb[slot(y, j), 288:320] for j in range(N)]
    part = jnp.concatenate(rows + [gb[1, 0:256]], 0).astype(bf16)
    gacc[...] = gacc[...] + mm(jnp.concatenate([wq[...], wk[...], wv[2]], 1), part)
    g_wide[1].wait()
    g_wide[3].wait()
    part = jnp.concatenate([gb[2, 0:256], gb[0, 0:256]], 0).astype(bf16)
    gacc[...] = gacc[...] + mm(jnp.concatenate([wv[0], wv[1]], 1), part)
    for i in range(16):
        gi[:, 128 * i : 128 * i + 128] = gacc[128 * i : 128 * i + 128].T.astype(bf16)
    out_copy = pltpu.make_async_copy(gi, gin.at[0], osem.at[0])
    out_copy.start()
    y_in.wait()
    for dy in range(N):
        rs[at_peer("seq_2", (4 - dy) % 4)] = yr[(dy + 3) % 4]
    lane = lax.broadcasted_iota(jnp.int32, (16, 128), 1) // 32
    w_q = jnp.zeros((16, 128), f32)
    w_k = jnp.zeros((16, 128), f32)
    for p in range(N):
        rs_v[:, 256 * p : 256 * p + 128] = rs[p, 0:16]
        rs_v[:, 256 * p + 128 : 256 * p + 256] = rs[p, 24:40]
        thin = rs[p, 16:24]
        thin = jnp.concatenate([thin, pltpu.roll(thin, 64, 1)], 0)
        from_q = pltpu.roll(thin, 32 * p, 1) if p else thin
        w_q = jnp.where(lane == p, from_q, w_q)
        from_k = pltpu.roll(thin, (32 * p + 96) % 128, 1) if p != 1 else thin
        w_k = jnp.where(lane == p, from_k, w_k)
    rs_q[...] = w_q
    rs_k[...] = w_k
    results = [out_copy]
    for i, (src, dst) in enumerate(((rs_q, gwq), (rs_k, gwk), (rs_v, gwv))):
        results.append(pltpu.make_async_copy(src, dst, osem.at[i + 1]))
        results[-1].start()
    for copy in results:
        copy.wait()
    assert groups[0] == GROUPS and bytes_sent[0] == SENT * 512
    to_pair.copy(total, total, {"batch": 1 - c}).wait_send()

    @pl.when(c == 1)
    def _():
        many = total.at[pl.ds(0, 4 * 256)]
        to_pair.copy(many, many, {"batch": 1 - c}, 1).wait_send()


def finish(*refs):
    sources, results, sems = refs[:4], refs[4:8], refs[8]
    copies = [
        pltpu.make_async_copy(src, dst, sems.at[i])
        for i, (src, dst) in enumerate(zip(sources, results))
    ]
    for copy in copies:
        copy.start()
    for copy in copies:
        copy.wait()


GROUPS = 3 + 6 + 4 * 3 + 1 + 1 + 4 + 4 + 1 + 4
SENT = (
    3 * 64 + 6 * 256 + 18 * 80 + 26 * 256 + 4 * 320 + 3 * 320
    + 12 * 96 + 12 * 64 + 3 * 96 + 3 * 64 + 3 * 40
)


def body(inputs, cotangent, w_query, w_key, w_value):
    vmem = pltpu.VMEM
    hbm = pl.BlockSpec(memory_space=pl.ANY)
    scan = [
        vmem((4, 80, 128), f32), vmem((4, 80, 128), f32), vmem((80, 128), f32),
        vmem((3, 80, 128), f32), vmem((4, 80, 128), f32), vmem((4, 80, 128), f32),
    ]
    scratch = [
        vmem((BLK, D), bf16), vmem((BLK, 1024), bf16), vmem((D, 128), bf16), vmem((D, 128), bf16),
        vmem((4, D, 256), bf16), vmem((2, 4, 256, 128), f32), vmem((4, 8, 256, 128), f32),
        vmem((4, 64, 128), f32), vmem((3, 128, 256), f32), vmem((4, 64, 128), f32),
        vmem((4, 128, 256), f32), vmem((4, 128, 256), f32), vmem((4, 128, 256), f32),
        vmem((2, FP, TOK), bf16), vmem((2, FP, TOK), bf16), vmem((2, TOK, 128), bf16),
        vmem((2, 128, TOK), bf16), vmem((2, 128, TOK), f32), vmem((2, TOK, TOK), bf16),
        vmem((2, 128, TOK), f32), vmem((2, 8, TOK), f32), vmem((2, 128, TOK), bf16),
        vmem((2, 8, TOK), f32), vmem((2, FP, TOK), f32), vmem((2, FP, TOK), f32),
        vmem((2, 128, TOK), f32), vmem((2, FP, 128), bf16), vmem((2, 8, FP), f32),
        *scan, *scan,
        vmem((2, 4, 320, 128), f32), vmem((4, 320, 128), f32), vmem((BLK, D), bf16),
        vmem((D, BLK), f32), vmem((4, 4, 96, 128), f32), vmem((4, 4, 64, 128), f32),
        vmem((4, 3, 96, 128), f32), vmem((2, 4, 64, 128), f32),
        vmem((4, 96, 128), f32), vmem((3, 96, 128), f32), vmem((3, 64, 128), f32),
        vmem((4, 64, 128), f32),
        vmem((4, 40, 128), f32), vmem((4, 40, 128), f32),
        vmem((4, 40, 128), f32), vmem((16, 128), f32), vmem((16, 128), f32),
        vmem((16, 1024), f32), vmem((SENT, 128), f32),
        pltpu.SemaphoreType.DMA((8,)), pltpu.SemaphoreType.DMA((4,)), pltpu.SemaphoreType.DMA((2,)),
        pltpu.SemaphoreType.DMA((GROUPS,)),
    ]
    shapes = (((1, BLK, D), bf16), ((16, 128), f32), ((16, 128), f32), ((16, 1024), f32))
    results = pl.pallas_call(
        kernel,
        out_shape=tuple(pltpu.VMEM(*shape) for shape in shapes),
        in_specs=[pl.BlockSpec(memory_space=pltpu.HBM)] * 5,
        out_specs=(hbm,) * 4,
        scratch_shapes=scratch,
        compiler_params=pltpu.CompilerParams(
            collective_id=0, has_side_effects=True, vmem_limit_bytes=60 * 1024 * 1024
        ),
    )(inputs, cotangent, w_query, w_key, w_value)
    return pl.pallas_call(
        finish,
        out_shape=tuple(jax.ShapeDtypeStruct(*shape) for shape in shapes),
        in_specs=[hbm] * 4,
        out_specs=(pl.BlockSpec(memory_space=pltpu.HBM),) * 4,
        scratch_shapes=[pltpu.SemaphoreType.DMA((4,))],
        compiler_params=pltpu.CompilerParams(vmem_limit_bytes=4 * 1024 * 1024),
    )(*results)


def solution(mesh):
    split = Mesh(
        mesh.devices.reshape(4, 4, 4, mesh.shape["batch"]), ("seq_0", "seq_1", "seq_2", "batch")
    )
    in_specs = (P("batch", SEQ, None), P("batch", SEQ, None), P(), P(), P())
    out_specs = (P("batch", SEQ, None), P(SEQ_BATCH, None), P(SEQ_BATCH, None), P(SEQ_BATCH, None))
    return jax.shard_map(body, mesh=split, in_specs=in_specs, out_specs=out_specs, check_vma=False)
```

```python
import math

import jax
import jax.numpy as jnp
from jax import lax
from jax.experimental import pallas as pl
from jax.experimental.pallas import tpu as pltpu
from jax.sharding import Mesh
from jax.sharding import PartitionSpec as P

D = 2048
H = 8
DK = 16
DV = 128
SEQ = ("seq_0", "seq_1", "seq_2")
SEQ_BATCH = ("seq_0", "seq_1", "seq_2", "batch")
N = 4
BLK = 128
TOK = N * BLK
FP = 160
ROOT = 1.0 / math.sqrt(2.0)
ORDER = (1, 3, 2, 0)
f32 = jnp.float32
bf16 = jnp.bfloat16
MESH_ID = pl.DeviceIdType.MESH


def mm(a, b):
    return lax.dot_general(a, b, (((1,), (0,)), ((), ())), preferred_element_type=f32)


def mm_nt(a, b):
    return lax.dot_general(a, b, (((1,), (1,)), ((), ())), preferred_element_type=f32)


def mm_tn(a, b):
    return lax.dot_general(a, b, (((0,), (0,)), ((), ())), preferred_element_type=f32)


def halves(row):
    high = row.astype(bf16).astype(f32)
    return high, row - high


def rows16(*rows):
    n = rows[0].shape[1]
    at = lax.broadcasted_iota(jnp.int32, (16, n), 0)
    out = jnp.zeros((16, n), f32)
    for i, row in enumerate(rows):
        out = jnp.where(at == i, jnp.broadcast_to(row, (16, n)), out)
    return out.astype(bf16)


def turned(u, d):
    d = d % DK
    return u if d == 0 else pltpu.roll(u, DK - d, 0)


def features(u):
    n = u.shape[1]
    parts = [u, u * u * ROOT]
    for d in range(1, 8):
        parts.append(u * turned(u, d))
    parts.append(u[:8] * u[8:])
    first = lax.broadcasted_iota(jnp.int32, (8, n), 0) == 0
    parts.append(jnp.where(first, 1.0, 0.0).astype(f32))
    return jnp.concatenate(parts, 0).astype(bf16)


def pull_back(u, g):
    out = g[0:16] + (g[16:32] * (2.0 * ROOT)) * u
    for d in range(1, 8):
        pair = g[16 + 16 * d : 32 + 16 * d]
        out = out + pair * turned(u, d) + turned(pair * u, -d)
    pair = g[144:152]
    return out + jnp.concatenate([pair * u[8:], pair * u[:8]], 0)


def kernel(
    x_hbm, u_hbm, wq_hbm, wk_hbm, wv_hbm,
    gin, gwq, gwk, gwv,
    xb, ub, wq, wk, wv, xt2, xg,
    sqk, sv, rqk, rv, us, ur,
    fq, fk, vb, vt, ut, at, num, dloc, gnb, gdr, gfq, gfk, gvt, stb, nrm,
    st1, xr1, zs1, zr1, pb1, pf1,
    st2, xr2, zs2, zr2, pb2, pf2,
    gg, gb, gacc, da, db, ra, rb, sa, fa, fb, fc, yb, yr, rs, total,
    lsem, ssem, rsem,
):
    z, x, y, c = (lax.axis_index(a) for a in SEQ_BATCH)
    place = {"seq_0": z, "seq_1": x, "seq_2": y}
    bytes_sent, groups = [0], [0]

    class Group:
        def __init__(self, like):
            self.like, self.k = like, groups[0]
            groups[0] += 1

        def copy(self, src, dst, target, k=0):
            return pltpu.make_async_remote_copy(
                src_ref=src, dst_ref=dst, send_sem=ssem.at[k], recv_sem=rsem.at[self.k],
                device_id=target, device_id_type=MESH_ID,
            )

        def send(self, src, dst, target, k=0):
            bytes_sent[0] += math.prod(src.shape) * 4 if k == 0 else 0
            self.copy(src, dst, target, k).start()

        def wait(self):
            self.copy(self.like, self.like, {"batch": 1 - c}).wait_recv()

    def one(src, dst, target):
        group = Group(dst)
        group.send(src, dst, target)
        return group

    def slot(place, j):
        return lax.rem(place - j + 7, N)

    def at_peer(axis, d):
        return lax.rem(place[axis] + d, N)

    loads = {}

    def load(name, k, src, dst):
        loads[name] = pltpu.make_async_copy(src, dst, lsem.at[k])
        loads[name].start()

    load("x", 0, x_hbm.at[0], xb)
    load("wq", 1, wq_hbm, wq)
    load("wk", 2, wk_hbm, wk)
    for k, dy in enumerate(ORDER):
        cols = pl.ds(pl.multiple_of(at_peer("seq_2", dy) * 256, 256), 256)
        load(("wv", k), 3 + k, wv_hbm.at[:, cols], wv.at[k])
    load("u", 7, u_hbm.at[0], ub)

    barrier = pltpu.get_barrier_semaphore()
    greeted = 0
    for d in range(N):
        for e in range(N):
            if d or e:
                greeted += 1
                pl.semaphore_signal(
                    barrier, inc=1, device_id_type=MESH_ID,
                    device_id={"seq_0": at_peer("seq_0", d), "seq_1": at_peer("seq_1", e)},
                )
        if d:
            greeted += 1
            pl.semaphore_signal(
                barrier, inc=1, device_id_type=MESH_ID, device_id={"seq_2": at_peer("seq_2", d)}
            )
        greeted += 1
        pl.semaphore_signal(
            barrier, inc=1, device_id_type=MESH_ID,
            device_id={"seq_2": at_peer("seq_2", d), "batch": 1 - c},
        )

    loads["x"].wait()
    loads["wq"].wait()
    qt = mm(xb[...], wq[...]).T
    loads["wk"].wait()
    kt = mm(xb[...], wk[...]).T
    for p in range(N):
        sqk[p, 0:32] = qt[32 * p : 32 * p + 32]
        sqk[p, 32:64] = kt[32 * p : 32 * p + 32]
    pl.semaphore_wait(barrier, greeted)
    qk_in = Group(rqk.at[pl.ds(0, 3)])
    for dy in (1, 3, 2):
        p = at_peer("seq_2", dy)
        qk_in.send(sqk.at[p], rqk.at[dy - 1], {"seq_2": p})
    rqk[3] = sqk[y]
    v_in = Group(rv.at[pl.ds(0, 3)])
    for k, dy in enumerate(ORDER):
        p = at_peer("seq_2", dy)
        loads[("wv", k)].wait()
        v = mm(xb[...], wv[k]).astype(bf16).astype(f32)
        if dy:
            sv[k] = v
            v_in.send(sv.at[k], rv.at[dy - 1], {"seq_2": p})
        else:
            rv[3] = v
    loads["u"].wait()
    for p in range(N):
        us[p] = ub[:, 256 * p : 256 * p + 256].astype(f32)
    u_in = Group(ur.at[pl.ds(0, 3)])
    for dy in (1, 3, 2):
        p = at_peer("seq_2", dy)
        u_in.send(us.at[p], ur.at[dy - 1], {"seq_2": p})
    ur[3] = us[y]

    for b in range(16):
        block = xb[:, 128 * b : 128 * b + 128].astype(f32).T
        for i in range(8):
            row = 64 * (b % 4) + 16 * (i // 2)
            xt2[i % 2, b // 4, row : row + 16] = block[16 * i : 16 * i + 16]
    chunk = [lax.rem(z + i + 1, N) for i in range(N)]
    after, before = at_peer("seq_2", 1), at_peer("seq_2", 3)
    x_in = [Group(xg.at[i, pl.ds(0, 5 if i < 3 else 4)]) for i in range(N)]
    passing = [None] * N

    def x_start(i):
        part = chunk[i]
        mine = xg.at[part, 2 * y + c]
        x_in[i].send(xt2.at[1 - c, part], mine, {"batch": 1 - c})
        up = one(xt2.at[c, part], mine, {"seq_2": after, "batch": c})
        x_in[i].send(xt2.at[c, part], mine, {"seq_2": before, "batch": c})
        x_in[i].send(xt2.at[1 - c, part], mine, {"seq_2": after, "batch": 1 - c})
        down = one(xt2.at[1 - c, part], mine, {"seq_2": before, "batch": 1 - c})
        xg[part, 2 * y + c] = xt2[c, part]
        passing[i] = (up, down)

    to_pair = one(xt2.at[1 - c, chunk[3]], xg.at[chunk[3], 2 * y + c], {"batch": 1 - c})
    xg[chunk[3], 2 * y + c] = xt2[c, chunk[3]]

    def x_start_last():
        part = chunk[3]
        mine = xg.at[part, 2 * y + c]
        up, down = Group(xg.at[3, 0]), Group(xg.at[3, 0])
        passing[3] = (up, down)
        up.send(xt2.at[c, part], mine, {"seq_2": after})
        x_in[3].send(xt2.at[c, part], mine, {"seq_2": before})
        to_pair.wait()

        @pl.when(c == 1)
        def _():
            for e in range(2):
                src = xg.at[part, 2 * y] if e else xt2.at[0, part]
                into = xg.at[part, 2 * y + 1 - e]
                x_in[3].send(src, into, {"seq_2": after, "batch": e}, 1)
                down.send(src, into, {"seq_2": before, "batch": e}, 1)

    def x_pass(i):
        part = chunk[i]
        up, down = passing[i]
        up.wait()
        move = xg.at[part, 2 * before + c]
        x_in[i].send(move, move, {"seq_2": after})
        down.wait()
        move = xg.at[part, 2 * after + 1 - c]
        x_in[i].send(move, move, {"seq_2": before})

    for i in range(N - 1):
        x_start(i)

    qk_in.wait()
    for h in range(2):
        lo = 16 * h
        uq = jnp.concatenate([rqk[slot(y, j), lo : lo + 16] for j in range(N)], 1) * 0.5
        uk = jnp.concatenate([rqk[slot(y, j), 32 + lo : 48 + lo] for j in range(N)], 1) * 0.5
        fq[h] = features(uq)
        fk[h] = features(uk)
    v_in.wait()
    ones = jnp.ones((16, TOK), bf16)
    for h in range(2):
        for j in range(N):
            vb[h, 128 * j : 128 * j + 128] = rv[slot(y, j), :, 128 * h : 128 * h + 128].astype(bf16)

    def put_state(st, h, state, norm):
        st[2 * h] = state[:80]
        st[2 * h + 1] = state[80:]
        st[2 * h + 1, 73:74] = norm[:, :128]
        st[2 * h + 1, 74:75] = jnp.concatenate([norm[:, 128:], jnp.zeros((1, 96), f32)], 1)

    def get_state(pf, h):
        low, high = slot(x, 2 * h), slot(x, 2 * h + 1)
        state = jnp.concatenate([pf[low], pf[high]], 0)
        norm = jnp.concatenate([pf[high, 73:74], pf[high, 74:75, :32]], 1)
        return state, norm

    for h in range(2):
        put_state(st1, h, mm(fk[h], vb[h]), mm_nt(ones, fk[h])[:1])

    def scan_start(st, xr):
        group = Group(xr.at[pl.ds(0, 3)])
        for d in (1, 3, 2):
            p = at_peer("seq_1", d)
            group.send(st.at[p], xr.at[d - 1], {"seq_1": p})
        xr[3] = st[x]
        return group

    def scan_mid(group, xr, zs, zr):
        group.wait()
        zs[...] = (xr[0] + xr[1]) + (xr[2] + xr[3])
        group = Group(zr)
        for d in (1, 3, 2):
            group.send(zs, zr.at[d - 1], {"seq_0": at_peer("seq_0", d)})
        return group

    def scan_back(group, xr, zr, pb, pf, later):
        group.wait()
        run = jnp.zeros((80, 128), f32)
        for d in (1, 2, 3):
            run = run + jnp.where(z < d if later else z >= d, zr[d - 1], 0.0)
        for i in reversed(range(N)) if later else range(N):
            pb[i] = run
            run = run + xr[slot(x, i)]
        group = Group(pf.at[pl.ds(0, 3)])
        for d in (1, 3, 2):
            p = at_peer("seq_1", d)
            group.send(pb.at[p], pf.at[d - 1], {"seq_1": p})
        pf[3] = pb[x]
        return group

    keep = lax.broadcasted_iota(jnp.int32, (TOK, TOK), 1) >= lax.broadcasted_iota(
        jnp.int32, (TOK, TOK), 0
    )

    def local_forward(h):
        for j in range(N):
            vt[h, :, 128 * j : 128 * j + 128] = (
                rv[slot(y, j), :, 128 * h : 128 * h + 128].T.astype(bf16)
            )
        scores = jnp.where(keep, mm_tn(fk[h], fq[h]), 0.0)
        dloc[h] = jnp.broadcast_to(jnp.sum(scores, 0, keepdims=True), (8, TOK))
        at[h] = scores.astype(bf16)
        num[h] = mm(vt[h], at[h])

    move = scan_start(st1, xr1)
    local_forward(0)
    move = scan_mid(move, xr1, zs1, zr1)
    local_forward(1)
    move = scan_back(move, xr1, zr1, pb1, pf1, False)
    u_in.wait()
    for h in range(2):
        for j in range(N):
            ut[h, :, 128 * j : 128 * j + 128] = ur[slot(y, j), :, 128 * h : 128 * h + 128].T
    move.wait()

    for h in range(2):
        state, norm = get_state(pf1, h)
        stb[h] = state.astype(bf16)
        n_hi, n_lo = halves(norm)
        nrm[h] = jnp.concatenate([n_hi, n_lo, n_hi, jnp.zeros((5, FP), f32)], 0)
        numer = num[h] + mm_tn(stb[h], fq[h])
        denom = dloc[h, :1] + jnp.sum(mm(rows16(n_hi, n_lo), fq[h]), 0, keepdims=True)
        inverse = 1.0 / denom
        upstream = ut[h]
        g_num = upstream * inverse
        g_den = -jnp.sum(upstream * (numer * inverse), 0, keepdims=True) * inverse
        gnb[h] = g_num.astype(bf16)
        g_hi, g_lo = halves(g_den)
        gdr[h] = jnp.concatenate([g_hi, g_lo, jnp.zeros((6, TOK), f32)], 0)
        back = mm_nt(fq[h], gnb[h])
        back_norm = jnp.sum(mm_nt(rows16(g_hi, g_lo), fq[h]), 0, keepdims=True)
        put_state(st2, h, back, back_norm)

    def local_backward(h):
        g_hi, g_lo = gdr[h, 0:1], gdr[h, 1:2]
        n_hi, n_lo = nrm[h, 0:1], nrm[h, 1:2]
        inner = mm(vb[h], gnb[h]) + (g_hi + g_lo)
        ga = jnp.where(keep, inner, 0.0).astype(bf16)
        outer = mm_tn(rows16(n_hi, n_lo, n_hi), rows16(g_hi, g_hi, g_lo))
        gfq[h] = mm(fk[h], ga) + mm(stb[h], gnb[h]) + outer
        gvt[h] = mm_nt(gnb[h], at[h])
        gfk[h] = mm_nt(fq[h], ga)

    def put_grad(h, first, u, grad):
        out = (pull_back(u, grad) * 0.5).astype(bf16).astype(f32)
        for j in range(N):
            gg[c, j, first + 16 * h : first + 16 * h + 16] = out[:, 128 * j : 128 * j + 128]

    move = scan_start(st2, xr2)
    x_pass(0)
    x_start_last()
    local_backward(0)
    move = scan_mid(move, xr2, zs2, zr2)
    x_pass(1)
    local_backward(1)
    move = scan_back(move, xr2, zr2, pb2, pf2, True)
    x_pass(2)
    for h in range(2):
        lo = 16 * h
        uq = jnp.concatenate([rqk[slot(y, j), lo : lo + 16] for j in range(N)], 1) * 0.5
        put_grad(h, 256, uq, gfq[h])
    move.wait()
    first16 = lax.broadcasted_iota(jnp.int32, (16, TOK), 0) < 2
    flag = jnp.where(first16, 1.0, 0.0).astype(bf16)
    for h in range(2):
        back, back_norm = get_state(pf2, h)
        backb = back.astype(bf16)
        b_hi, b_lo = halves(back_norm)
        g_val = gvt[h] + mm_tn(backb, fk[h])
        g_val = g_val.astype(bf16).astype(f32)
        for j in range(N):
            gg[c, j, 128 * h : 128 * h + 128] = g_val[:, 128 * j : 128 * j + 128]
        g_fk = gfk[h] + mm(backb, vt[h]) + mm_tn(rows16(b_hi, b_lo), flag)
        lo = 32 + 16 * h
        uk = jnp.concatenate([rqk[slot(y, j), lo : lo + 16] for j in range(N)], 1) * 0.5
        put_grad(h, 288, uk, g_fk)

    pair_g = one(gg.at[c], gg.at[c], {"batch": 1 - c})
    pair_g.wait()
    rhs = jnp.concatenate([gg[i, j].astype(bf16) for j in range(N) for i in range(2)], 1)

    a_in = [Group(ra.at[i]) for i in range(N)]
    b_in, c_last = Group(rb), Group(fc)

    def weights_of(i):
        part = chunk[i]
        lhs = jnp.concatenate(
            [xg[part, j].astype(bf16) for j in range(8)], 1
        )
        out = mm_nt(lhs, rhs)
        for xx in range(N):
            for j in range(N):
                own = out[64 * xx + 16 * j : 64 * xx + 16 * j + 16]
                thin = own[:, 256:320]
                da[i, xx, 24 * j : 24 * j + 16] = own[:, :128]
                da[i, xx, 24 * j + 16 : 24 * j + 24] = jnp.concatenate([thin[:8], thin[8:]], 1)
                db[i, xx, 16 * j : 16 * j + 16] = own[:, 128:256]
        for k, d in enumerate((1, 3, 2)):
            p = at_peer("seq_1", d)
            a_in[i].send(da.at[i, p], ra.at[i, k], {"seq_1": p})
        if i < 2:
            b_in.send(db.at[i], rb.at[i], {"seq_0": part})
        elif i == 2:
            for d in (1, 3, 2, 0):
                p = at_peer("seq_1", d)
                c_last.send(db.at[i, p], fc.at[(d + 3) % 4], {"seq_0": part, "seq_1": p})

    a_last, b_last = Group(fa), Group(fb)

    def a_onward(i):
        a_in[i].wait()
        sa[i] = (da[i, x] + ra[i, 0]) + (ra[i, 1] + ra[i, 2])
        if i < N - 1:
            a_last.send(sa.at[i], fa.at[i], {"seq_0": chunk[i]})

    x_in[0].wait()
    weights_of(0)
    x_pass(3)
    x_in[1].wait()
    weights_of(1)
    x_in[2].wait()
    weights_of(2)
    g_thin = Group(gb.at[pl.ds(0, 3), pl.ds(256, 64)])
    a_onward(0)
    gb[3] = gg[c, y]
    gacc[...] = mm(wv[3], gb[3, 0:256].astype(bf16))
    x_in[3].wait()
    g_wide = {}
    for dy in (2, 1, 3):
        p = at_peer("seq_2", dy)
        g_thin.send(gg.at[c, p, pl.ds(256, 64)], gb.at[dy - 1, pl.ds(256, 64)], {"seq_2": p})
    for dy in (2, 1, 3):
        p = at_peer("seq_2", dy)
        g_wide[dy] = one(gg.at[c, p, pl.ds(0, 256)], gb.at[dy - 1, pl.ds(0, 256)], {"seq_2": p})
    weights_of(3)
    b_in.wait()
    for xx in range(N):
        db[3, xx] = db[3, xx] + (rb[0, xx] + rb[1, xx])
    for d in (1, 3, 2):
        p = at_peer("seq_1", d)
        b_last.send(db.at[3, p], fb.at[d - 1], {"seq_1": p})
    a_onward(1)
    a_onward(2)

    a_onward(3)
    a_last.wait()
    b_last.wait()
    c_last.wait()
    sum_a = (sa[3] + fa[0]) + (fa[1] + fa[2])
    sum_b = (db[3, x] + fb[0]) + (fb[1] + fb[2])
    sum_b = sum_b + ((fc[0] + fc[1]) + (fc[2] + fc[3]))
    for j in range(N):
        yb[j, 0:24] = sum_a[24 * j : 24 * j + 24]
        yb[j, 24:40] = sum_b[16 * j : 16 * j + 16]
    y_in = Group(yr.at[pl.ds(0, 3)])
    for dy in (2, 1, 3):
        p = at_peer("seq_2", dy)
        y_in.send(yb.at[p], yr.at[dy - 1], {"seq_2": p})
    yr[3] = yb[y]
    g_thin.wait()
    g_wide[2].wait()
    rows = [gb[slot(y, j), 256:288] for j in range(N)] + [gb[slot(y, j), 288:320] for j in range(N)]
    part = jnp.concatenate(rows + [gb[1, 0:256]], 0).astype(bf16)
    gacc[...] = gacc[...] + mm(jnp.concatenate([wq[...], wk[...], wv[2]], 1), part)
    g_wide[1].wait()
    g_wide[3].wait()
    part = jnp.concatenate([gb[2, 0:256], gb[0, 0:256]], 0).astype(bf16)
    gacc[...] = gacc[...] + mm(jnp.concatenate([wv[0], wv[1]], 1), part)
    for i in range(16):
        gin[0, :, 128 * i : 128 * i + 128] = gacc[128 * i : 128 * i + 128].T.astype(bf16)
    y_in.wait()
    for dy in range(N):
        rs[at_peer("seq_2", (4 - dy) % 4)] = yr[(dy + 3) % 4]
    lane = lax.broadcasted_iota(jnp.int32, (16, 128), 1) // 32
    w_q = jnp.zeros((16, 128), f32)
    w_k = jnp.zeros((16, 128), f32)
    for p in range(N):
        gwv[:, 256 * p : 256 * p + 128] = rs[p, 0:16]
        gwv[:, 256 * p + 128 : 256 * p + 256] = rs[p, 24:40]
        thin = rs[p, 16:24]
        thin = jnp.concatenate([thin, pltpu.roll(thin, 64, 1)], 0)
        from_q = pltpu.roll(thin, 32 * p, 1) if p else thin
        w_q = jnp.where(lane == p, from_q, w_q)
        from_k = pltpu.roll(thin, (32 * p + 96) % 128, 1) if p != 1 else thin
        w_k = jnp.where(lane == p, from_k, w_k)
    gwq[...] = w_q
    gwk[...] = w_k
    assert groups[0] == GROUPS and bytes_sent[0] == SENT * 512
    to_pair.copy(total, total, {"batch": 1 - c}).wait_send()

    @pl.when(c == 1)
    def _():
        many = total.at[pl.ds(0, 4 * 256)]
        to_pair.copy(many, many, {"batch": 1 - c}, 1).wait_send()


def finish(*refs):
    sources, results, sems = refs[:4], refs[4:8], refs[8]
    copies = [
        pltpu.make_async_copy(src, dst, sems.at[i])
        for i, (src, dst) in enumerate(zip(sources, results))
    ]
    for copy in copies:
        copy.start()
    for copy in copies:
        copy.wait()


GROUPS = 3 + 6 + 4 * 3 + 1 + 1 + 4 + 4 + 1 + 4
SENT = (
    3 * 64 + 6 * 256 + 18 * 80 + 26 * 256 + 4 * 320 + 3 * 320
    + 12 * 96 + 12 * 64 + 3 * 96 + 3 * 64 + 3 * 40
)


def body(inputs, cotangent, w_query, w_key, w_value):
    vmem = pltpu.VMEM
    hbm = pl.BlockSpec(memory_space=pl.ANY)
    scan = [
        vmem((4, 80, 128), f32), vmem((4, 80, 128), f32), vmem((80, 128), f32),
        vmem((3, 80, 128), f32), vmem((4, 80, 128), f32), vmem((4, 80, 128), f32),
    ]
    scratch = [
        vmem((BLK, D), bf16), vmem((BLK, 1024), bf16), vmem((D, 128), bf16), vmem((D, 128), bf16),
        vmem((4, D, 256), bf16), vmem((2, 4, 256, 128), f32), vmem((4, 8, 256, 128), f32),
        vmem((4, 64, 128), f32), vmem((3, 128, 256), f32), vmem((4, 64, 128), f32),
        vmem((4, 128, 256), f32), vmem((4, 128, 256), f32), vmem((4, 128, 256), f32),
        vmem((2, FP, TOK), bf16), vmem((2, FP, TOK), bf16), vmem((2, TOK, 128), bf16),
        vmem((2, 128, TOK), bf16), vmem((2, 128, TOK), f32), vmem((2, TOK, TOK), bf16),
        vmem((2, 128, TOK), f32), vmem((2, 8, TOK), f32), vmem((2, 128, TOK), bf16),
        vmem((2, 8, TOK), f32), vmem((2, FP, TOK), f32), vmem((2, FP, TOK), f32),
        vmem((2, 128, TOK), f32), vmem((2, FP, 128), bf16), vmem((2, 8, FP), f32),
        *scan, *scan,
        vmem((2, 4, 320, 128), f32), vmem((4, 320, 128), f32),
        vmem((D, BLK), f32), vmem((4, 4, 96, 128), f32), vmem((4, 4, 64, 128), f32),
        vmem((4, 3, 96, 128), f32), vmem((2, 4, 64, 128), f32),
        vmem((4, 96, 128), f32), vmem((3, 96, 128), f32), vmem((3, 64, 128), f32),
        vmem((4, 64, 128), f32),
        vmem((4, 40, 128), f32), vmem((4, 40, 128), f32),
        vmem((4, 40, 128), f32), vmem((SENT, 128), f32),
        pltpu.SemaphoreType.DMA((8,)), pltpu.SemaphoreType.DMA((2,)),
        pltpu.SemaphoreType.DMA((GROUPS,)),
    ]
    shapes = (((1, BLK, D), bf16), ((16, 128), f32), ((16, 128), f32), ((16, 1024), f32))
    results = pl.pallas_call(
        kernel,
        out_shape=tuple(pltpu.VMEM(*shape) for shape in shapes),
        in_specs=[pl.BlockSpec(memory_space=pltpu.HBM)] * 5,
        out_specs=(pl.BlockSpec(memory_space=pltpu.VMEM),) * 4,
        scratch_shapes=scratch,
        compiler_params=pltpu.CompilerParams(
            collective_id=0, has_side_effects=True, vmem_limit_bytes=60 * 1024 * 1024
        ),
    )(inputs, cotangent, w_query, w_key, w_value)
    return pl.pallas_call(
        finish,
        out_shape=tuple(jax.ShapeDtypeStruct(*shape) for shape in shapes),
        in_specs=[hbm] * 4,
        out_specs=(pl.BlockSpec(memory_space=pltpu.HBM),) * 4,
        scratch_shapes=[pltpu.SemaphoreType.DMA((4,))],
        compiler_params=pltpu.CompilerParams(vmem_limit_bytes=4 * 1024 * 1024),
    )(*results)


def solution(mesh):
    split = Mesh(
        mesh.devices.reshape(4, 4, 4, mesh.shape["batch"]), ("seq_0", "seq_1", "seq_2", "batch")
    )
    in_specs = (P("batch", SEQ, None), P("batch", SEQ, None), P(), P(), P())
    out_specs = (P("batch", SEQ, None), P(SEQ_BATCH, None), P(SEQ_BATCH, None), P(SEQ_BATCH, None))
    return jax.shard_map(body, mesh=split, in_specs=in_specs, out_specs=out_specs, check_vma=False)
```

```python
import math

import jax
import jax.numpy as jnp
from jax import lax
from jax.experimental import pallas as pl
from jax.experimental.pallas import tpu as pltpu
from jax.sharding import Mesh
from jax.sharding import PartitionSpec as P

D = 2048
H = 8
DK = 16
DV = 128
SEQ = ("seq_0", "seq_1", "seq_2")
SEQ_BATCH = ("seq_0", "seq_1", "seq_2", "batch")
N = 4
BLK = 128
TOK = N * BLK
FP = 160
ROOT = 1.0 / math.sqrt(2.0)
ORDER = (1, 3, 2, 0)
f32 = jnp.float32
bf16 = jnp.bfloat16
MESH_ID = pl.DeviceIdType.MESH


def mm(a, b):
    return lax.dot_general(a, b, (((1,), (0,)), ((), ())), preferred_element_type=f32)


def mm_nt(a, b):
    return lax.dot_general(a, b, (((1,), (1,)), ((), ())), preferred_element_type=f32)


def mm_tn(a, b):
    return lax.dot_general(a, b, (((0,), (0,)), ((), ())), preferred_element_type=f32)


def halves(row):
    high = row.astype(bf16).astype(f32)
    return high, row - high


def rows16(*rows):
    n = rows[0].shape[1]
    at = lax.broadcasted_iota(jnp.int32, (16, n), 0)
    out = jnp.zeros((16, n), f32)
    for i, row in enumerate(rows):
        out = jnp.where(at == i, jnp.broadcast_to(row, (16, n)), out)
    return out.astype(bf16)


def turned(u, d):
    d = d % DK
    return u if d == 0 else pltpu.roll(u, DK - d, 0)


def features(u):
    n = u.shape[1]
    parts = [u, u * u * ROOT]
    for d in range(1, 8):
        parts.append(u * turned(u, d))
    parts.append(u[:8] * u[8:])
    first = lax.broadcasted_iota(jnp.int32, (8, n), 0) == 0
    parts.append(jnp.where(first, 1.0, 0.0).astype(f32))
    return jnp.concatenate(parts, 0).astype(bf16)


def pull_back(u, g):
    out = g[0:16] + (g[16:32] * (2.0 * ROOT)) * u
    for d in range(1, 8):
        pair = g[16 + 16 * d : 32 + 16 * d]
        out = out + pair * turned(u, d) + turned(pair * u, -d)
    pair = g[144:152]
    return out + jnp.concatenate([pair * u[8:], pair * u[:8]], 0)


def kernel(
    x_hbm, u_hbm, wq_hbm, wk_hbm, wv_hbm,
    gin, gwq, gwk, gwv,
    xb, ub, wq, wk, wv, xt2, xg,
    sqk, sv, rqk, rv, us, ur,
    fq, fk, vb, vt, ut, at, num, dloc, gnb, gdr, gfq, gfk, gvt, stb, nrm,
    st1, xr1, zs1, zr1, pb1, pf1,
    st2, xr2, zs2, zr2, pb2, pf2,
    gg, gb, gacc, da, db, ra, rb, sa, fa, fb, fc, yb, yr, rs, total,
    lsem, ssem, rsem,
):
    z, x, y, c = (lax.axis_index(a) for a in SEQ_BATCH)
    place = {"seq_0": z, "seq_1": x, "seq_2": y}
    bytes_sent, groups = [0], [0]

    class Group:
        def __init__(self, like):
            self.like, self.k = like, groups[0]
            groups[0] += 1

        def copy(self, src, dst, target, k=0):
            return pltpu.make_async_remote_copy(
                src_ref=src, dst_ref=dst, send_sem=ssem.at[k], recv_sem=rsem.at[self.k],
                device_id=target, device_id_type=MESH_ID,
            )

        def send(self, src, dst, target, k=0):
            bytes_sent[0] += math.prod(src.shape) * 4 if k == 0 else 0
            self.copy(src, dst, target, k).start()

        def wait(self):
            self.copy(self.like, self.like, {"batch": 1 - c}).wait_recv()

    def one(src, dst, target):
        group = Group(dst)
        group.send(src, dst, target)
        return group

    def slot(place, j):
        return lax.rem(place - j + 7, N)

    def at_peer(axis, d):
        return lax.rem(place[axis] + d, N)

    loads = {}

    def load(name, k, src, dst):
        loads[name] = pltpu.make_async_copy(src, dst, lsem.at[k])
        loads[name].start()

    load("x", 0, x_hbm.at[0], xb)
    load("wq", 1, wq_hbm, wq)
    load("wk", 2, wk_hbm, wk)
    for k, dy in enumerate(ORDER):
        cols = pl.ds(pl.multiple_of(at_peer("seq_2", dy) * 256, 256), 256)
        load(("wv", k), 3 + k, wv_hbm.at[:, cols], wv.at[k])
    load("u", 7, u_hbm.at[0], ub)

    barrier = pltpu.get_barrier_semaphore()
    greeted = 0
    for d in range(N):
        for e in range(N):
            if d or e:
                greeted += 1
                pl.semaphore_signal(
                    barrier, inc=1, device_id_type=MESH_ID,
                    device_id={"seq_0": at_peer("seq_0", d), "seq_1": at_peer("seq_1", e)},
                )
        if d:
            greeted += 1
            pl.semaphore_signal(
                barrier, inc=1, device_id_type=MESH_ID, device_id={"seq_2": at_peer("seq_2", d)}
            )
        greeted += 1
        pl.semaphore_signal(
            barrier, inc=1, device_id_type=MESH_ID,
            device_id={"seq_2": at_peer("seq_2", d), "batch": 1 - c},
        )

    loads["x"].wait()
    loads["wq"].wait()
    qt = mm(xb[...], wq[...]).T
    loads["wk"].wait()
    kt = mm(xb[...], wk[...]).T
    for p in range(N):
        sqk[p, 0:32] = qt[32 * p : 32 * p + 32]
        sqk[p, 32:64] = kt[32 * p : 32 * p + 32]
    pl.semaphore_wait(barrier, greeted)
    qk_in = Group(rqk.at[pl.ds(0, 3)])
    for dy in (1, 3, 2):
        p = at_peer("seq_2", dy)
        qk_in.send(sqk.at[p], rqk.at[dy - 1], {"seq_2": p})
    rqk[3] = sqk[y]
    v_in = Group(rv.at[pl.ds(0, 3)])
    for k, dy in enumerate(ORDER):
        p = at_peer("seq_2", dy)
        loads[("wv", k)].wait()
        v = mm(xb[...], wv[k]).astype(bf16).astype(f32)
        if dy:
            sv[k] = v
            v_in.send(sv.at[k], rv.at[dy - 1], {"seq_2": p})
        else:
            rv[3] = v
    loads["u"].wait()
    for p in range(N):
        us[p] = ub[:, 256 * p : 256 * p + 256].astype(f32)
    u_in = Group(ur.at[pl.ds(0, 3)])
    for dy in (1, 3, 2):
        p = at_peer("seq_2", dy)
        u_in.send(us.at[p], ur.at[dy - 1], {"seq_2": p})
    ur[3] = us[y]

    for b in range(16):
        block = xb[:, 128 * b : 128 * b + 128].astype(f32).T
        for i in range(8):
            row = 64 * (b % 4) + 16 * (i // 2)
            xt2[i % 2, b // 4, row : row + 16] = block[16 * i : 16 * i + 16]
    chunk = [lax.rem(z + i + 1, N) for i in range(N)]
    after, before = at_peer("seq_2", 1), at_peer("seq_2", 3)
    x_in = [Group(xg.at[i, pl.ds(0, 5 if i < 3 else 4)]) for i in range(N)]
    passing = [None] * N

    def x_start(i):
        part = chunk[i]
        mine = xg.at[part, 2 * y + c]
        x_in[i].send(xt2.at[1 - c, part], mine, {"batch": 1 - c})
        up = one(xt2.at[c, part], mine, {"seq_2": after, "batch": c})
        x_in[i].send(xt2.at[c, part], mine, {"seq_2": before, "batch": c})
        x_in[i].send(xt2.at[1 - c, part], mine, {"seq_2": after, "batch": 1 - c})
        down = one(xt2.at[1 - c, part], mine, {"seq_2": before, "batch": 1 - c})
        xg[part, 2 * y + c] = xt2[c, part]
        passing[i] = (up, down)

    to_pair = one(xt2.at[1 - c, chunk[3]], xg.at[chunk[3], 2 * y + c], {"batch": 1 - c})
    xg[chunk[3], 2 * y + c] = xt2[c, chunk[3]]

    def x_start_last():
        part = chunk[3]
        mine = xg.at[part, 2 * y + c]
        up, down = Group(xg.at[3, 0]), Group(xg.at[3, 0])
        passing[3] = (up, down)
        up.send(xt2.at[c, part], mine, {"seq_2": after})
        x_in[3].send(xt2.at[c, part], mine, {"seq_2": before})
        to_pair.wait()

        @pl.when(c == 1)
        def _():
            for e in range(2):
                src = xg.at[part, 2 * y] if e else xt2.at[0, part]
                into = xg.at[part, 2 * y + 1 - e]
                x_in[3].send(src, into, {"seq_2": after, "batch": e}, 1)
                down.send(src, into, {"seq_2": before, "batch": e}, 1)

    def x_pass(i):
        part = chunk[i]
        up, down = passing[i]
        up.wait()
        move = xg.at[part, 2 * before + c]
        x_in[i].send(move, move, {"seq_2": after})
        down.wait()
        move = xg.at[part, 2 * after + 1 - c]
        x_in[i].send(move, move, {"seq_2": before})

    for i in range(N - 1):
        x_start(i)

    qk_in.wait()
    for h in range(2):
        lo = 16 * h
        uq = jnp.concatenate([rqk[slot(y, j), lo : lo + 16] for j in range(N)], 1) * 0.5
        uk = jnp.concatenate([rqk[slot(y, j), 32 + lo : 48 + lo] for j in range(N)], 1) * 0.5
        fq[h] = features(uq)
        fk[h] = features(uk)
    v_in.wait()
    ones = jnp.ones((16, TOK), bf16)
    for h in range(2):
        for j in range(N):
            vb[h, 128 * j : 128 * j + 128] = rv[slot(y, j), :, 128 * h : 128 * h + 128].astype(bf16)

    def put_state(st, h, state, norm):
        st[2 * h] = state[:80]
        st[2 * h + 1] = state[80:]
        st[2 * h + 1, 73:74] = norm[:, :128]
        st[2 * h + 1, 74:75] = jnp.concatenate([norm[:, 128:], jnp.zeros((1, 96), f32)], 1)

    def get_state(pf, h):
        low, high = slot(x, 2 * h), slot(x, 2 * h + 1)
        state = jnp.concatenate([pf[low], pf[high]], 0)
        norm = jnp.concatenate([pf[high, 73:74], pf[high, 74:75, :32]], 1)
        return state, norm

    for h in range(2):
        put_state(st1, h, mm(fk[h], vb[h]), mm_nt(ones, fk[h])[:1])

    def scan_start(st, xr):
        group = Group(xr.at[pl.ds(0, 3)])
        for d in (1, 3, 2):
            p = at_peer("seq_1", d)
            group.send(st.at[p], xr.at[d - 1], {"seq_1": p})
        xr[3] = st[x]
        return group

    def scan_mid(group, xr, zs, zr):
        group.wait()
        zs[...] = (xr[0] + xr[1]) + (xr[2] + xr[3])
        group = Group(zr)
        for d in (1, 3, 2):
            group.send(zs, zr.at[d - 1], {"seq_0": at_peer("seq_0", d)})
        return group

    def scan_back(group, xr, zr, pb, pf, later):
        group.wait()
        run = jnp.zeros((80, 128), f32)
        for d in (1, 2, 3):
            run = run + jnp.where(z < d if later else z >= d, zr[d - 1], 0.0)
        for i in reversed(range(N)) if later else range(N):
            pb[i] = run
            run = run + xr[slot(x, i)]
        group = Group(pf.at[pl.ds(0, 3)])
        for d in (1, 3, 2):
            p = at_peer("seq_1", d)
            group.send(pb.at[p], pf.at[d - 1], {"seq_1": p})
        pf[3] = pb[x]
        return group

    keep = lax.broadcasted_iota(jnp.int32, (TOK, TOK), 1) >= lax.broadcasted_iota(
        jnp.int32, (TOK, TOK), 0
    )

    def local_forward(h):
        for j in range(N):
            vt[h, :, 128 * j : 128 * j + 128] = (
                rv[slot(y, j), :, 128 * h : 128 * h + 128].T.astype(bf16)
            )
        scores = jnp.where(keep, mm_tn(fk[h], fq[h]), 0.0)
        dloc[h] = jnp.broadcast_to(jnp.sum(scores, 0, keepdims=True), (8, TOK))
        at[h] = scores.astype(bf16)
        num[h] = mm(vt[h], at[h])

    move = scan_start(st1, xr1)
    local_forward(0)
    move = scan_mid(move, xr1, zs1, zr1)
    local_forward(1)
    move = scan_back(move, xr1, zr1, pb1, pf1, False)
    u_in.wait()
    for h in range(2):
        for j in range(N):
            ut[h, :, 128 * j : 128 * j + 128] = ur[slot(y, j), :, 128 * h : 128 * h + 128].T
    move.wait()

    for h in range(2):
        state, norm = get_state(pf1, h)
        stb[h] = state.astype(bf16)
        n_hi, n_lo = halves(norm)
        nrm[h] = jnp.concatenate([n_hi, n_lo, n_hi, jnp.zeros((5, FP), f32)], 0)
        numer = num[h] + mm_tn(stb[h], fq[h])
        denom = dloc[h, :1] + jnp.sum(mm(rows16(n_hi, n_lo), fq[h]), 0, keepdims=True)
        inverse = 1.0 / denom
        upstream = ut[h]
        g_num = upstream * inverse
        g_den = -jnp.sum(upstream * (numer * inverse), 0, keepdims=True) * inverse
        gnb[h] = g_num.astype(bf16)
        g_hi, g_lo = halves(g_den)
        gdr[h] = jnp.concatenate([g_hi, g_lo, jnp.zeros((6, TOK), f32)], 0)
        back = mm_nt(fq[h], gnb[h])
        back_norm = jnp.sum(mm_nt(rows16(g_hi, g_lo), fq[h]), 0, keepdims=True)
        put_state(st2, h, back, back_norm)

    def local_backward(h):
        g_hi, g_lo = gdr[h, 0:1], gdr[h, 1:2]
        n_hi, n_lo = nrm[h, 0:1], nrm[h, 1:2]
        inner = mm(vb[h], gnb[h]) + (g_hi + g_lo)
        ga = jnp.where(keep, inner, 0.0).astype(bf16)
        outer = mm_tn(rows16(n_hi, n_lo, n_hi), rows16(g_hi, g_hi, g_lo))
        gfq[h] = mm(fk[h], ga) + mm(stb[h], gnb[h]) + outer
        gvt[h] = mm_nt(gnb[h], at[h])
        gfk[h] = mm_nt(fq[h], ga)

    def put_grad(h, first, u, grad):
        out = (pull_back(u, grad) * 0.5).astype(bf16).astype(f32)
        for j in range(N):
            gg[c, j, first + 16 * h : first + 16 * h + 16] = out[:, 128 * j : 128 * j + 128]

    move = scan_start(st2, xr2)
    x_pass(0)
    x_start_last()
    local_backward(0)
    move = scan_mid(move, xr2, zs2, zr2)
    x_pass(1)
    local_backward(1)
    move = scan_back(move, xr2, zr2, pb2, pf2, True)
    x_pass(2)
    for h in range(2):
        lo = 16 * h
        uq = jnp.concatenate([rqk[slot(y, j), lo : lo + 16] for j in range(N)], 1) * 0.5
        put_grad(h, 256, uq, gfq[h])
    move.wait()
    first16 = lax.broadcasted_iota(jnp.int32, (16, TOK), 0) < 2
    flag = jnp.where(first16, 1.0, 0.0).astype(bf16)
    for h in range(2):
        back, back_norm = get_state(pf2, h)
        backb = back.astype(bf16)
        b_hi, b_lo = halves(back_norm)
        g_val = gvt[h] + mm_tn(backb, fk[h])
        g_val = g_val.astype(bf16).astype(f32)
        for j in range(N):
            gg[c, j, 128 * h : 128 * h + 128] = g_val[:, 128 * j : 128 * j + 128]
        g_fk = gfk[h] + mm(backb, vt[h]) + mm_tn(rows16(b_hi, b_lo), flag)
        lo = 32 + 16 * h
        uk = jnp.concatenate([rqk[slot(y, j), lo : lo + 16] for j in range(N)], 1) * 0.5
        put_grad(h, 288, uk, g_fk)

    pair_g = one(gg.at[c], gg.at[c], {"batch": 1 - c})
    gb[3] = gg[c, y]
    gacc[...] = mm(wv[3], gb[3, 0:256].astype(bf16))
    pair_g.wait()
    rhs = jnp.concatenate([gg[i, j].astype(bf16) for j in range(N) for i in range(2)], 1)

    a_in = [Group(ra.at[i]) for i in range(N)]
    b_in, c_last = Group(rb), Group(fc)

    def weights_of(i):
        part = chunk[i]
        lhs = jnp.concatenate(
            [xg[part, j].astype(bf16) for j in range(8)], 1
        )
        out = mm_nt(lhs, rhs)
        for xx in range(N):
            for j in range(N):
                own = out[64 * xx + 16 * j : 64 * xx + 16 * j + 16]
                thin = own[:, 256:320]
                da[i, xx, 24 * j : 24 * j + 16] = own[:, :128]
                da[i, xx, 24 * j + 16 : 24 * j + 24] = jnp.concatenate([thin[:8], thin[8:]], 1)
                db[i, xx, 16 * j : 16 * j + 16] = own[:, 128:256]
        for k, d in enumerate((1, 3, 2)):
            p = at_peer("seq_1", d)
            a_in[i].send(da.at[i, p], ra.at[i, k], {"seq_1": p})
        if i < 2:
            b_in.send(db.at[i], rb.at[i], {"seq_0": part})
        elif i == 2:
            for d in (1, 3, 2, 0):
                p = at_peer("seq_1", d)
                c_last.send(db.at[i, p], fc.at[(d + 3) % 4], {"seq_0": part, "seq_1": p})

    a_last, b_last = Group(fa), Group(fb)

    def a_onward(i):
        a_in[i].wait()
        sa[i] = (da[i, x] + ra[i, 0]) + (ra[i, 1] + ra[i, 2])
        if i < N - 1:
            a_last.send(sa.at[i], fa.at[i], {"seq_0": chunk[i]})

    x_in[0].wait()
    weights_of(0)
    x_pass(3)
    x_in[1].wait()
    weights_of(1)
    x_in[2].wait()
    weights_of(2)
    g_thin = Group(gb.at[pl.ds(0, 3), pl.ds(256, 64)])
    a_onward(0)
    x_in[3].wait()
    g_wide = {}
    for dy in (2, 1, 3):
        p = at_peer("seq_2", dy)
        g_thin.send(gg.at[c, p, pl.ds(256, 64)], gb.at[dy - 1, pl.ds(256, 64)], {"seq_2": p})
    for dy in (2, 1, 3):
        p = at_peer("seq_2", dy)
        g_wide[dy] = one(gg.at[c, p, pl.ds(0, 256)], gb.at[dy - 1, pl.ds(0, 256)], {"seq_2": p})
    weights_of(3)
    a_onward(1)
    b_in.wait()
    for xx in range(N):
        db[3, xx] = db[3, xx] + (rb[0, xx] + rb[1, xx])
    for d in (1, 3, 2):
        p = at_peer("seq_1", d)
        b_last.send(db.at[3, p], fb.at[d - 1], {"seq_1": p})
    a_onward(2)

    a_onward(3)
    a_last.wait()
    b_last.wait()
    c_last.wait()
    sum_a = (sa[3] + fa[0]) + (fa[1] + fa[2])
    sum_b = (db[3, x] + fb[0]) + (fb[1] + fb[2])
    sum_b = sum_b + ((fc[0] + fc[1]) + (fc[2] + fc[3]))
    for j in range(N):
        yb[j, 0:24] = sum_a[24 * j : 24 * j + 24]
        yb[j, 24:40] = sum_b[16 * j : 16 * j + 16]
    y_in = Group(yr.at[pl.ds(0, 3)])
    for dy in (2, 1, 3):
        p = at_peer("seq_2", dy)
        y_in.send(yb.at[p], yr.at[dy - 1], {"seq_2": p})
    yr[3] = yb[y]
    g_thin.wait()
    g_wide[2].wait()
    rows = [gb[slot(y, j), 256:288] for j in range(N)] + [gb[slot(y, j), 288:320] for j in range(N)]
    part = jnp.concatenate(rows + [gb[1, 0:256]], 0).astype(bf16)
    gacc[...] = gacc[...] + mm(jnp.concatenate([wq[...], wk[...], wv[2]], 1), part)
    g_wide[1].wait()
    g_wide[3].wait()
    part = jnp.concatenate([gb[2, 0:256], gb[0, 0:256]], 0).astype(bf16)
    gacc[...] = gacc[...] + mm(jnp.concatenate([wv[0], wv[1]], 1), part)
    for i in range(16):
        gin[0, :, 128 * i : 128 * i + 128] = gacc[128 * i : 128 * i + 128].T.astype(bf16)
    y_in.wait()
    for dy in range(N):
        rs[at_peer("seq_2", (4 - dy) % 4)] = yr[(dy + 3) % 4]
    lane = lax.broadcasted_iota(jnp.int32, (16, 128), 1) // 32
    w_q = jnp.zeros((16, 128), f32)
    w_k = jnp.zeros((16, 128), f32)
    for p in range(N):
        gwv[:, 256 * p : 256 * p + 128] = rs[p, 0:16]
        gwv[:, 256 * p + 128 : 256 * p + 256] = rs[p, 24:40]
        thin = rs[p, 16:24]
        thin = jnp.concatenate([thin, pltpu.roll(thin, 64, 1)], 0)
        from_q = pltpu.roll(thin, 32 * p, 1) if p else thin
        w_q = jnp.where(lane == p, from_q, w_q)
        from_k = pltpu.roll(thin, (32 * p + 96) % 128, 1) if p != 1 else thin
        w_k = jnp.where(lane == p, from_k, w_k)
    gwq[...] = w_q
    gwk[...] = w_k
    assert groups[0] == GROUPS and bytes_sent[0] == SENT * 512
    to_pair.copy(total, total, {"batch": 1 - c}).wait_send()

    @pl.when(c == 1)
    def _():
        many = total.at[pl.ds(0, 4 * 256)]
        to_pair.copy(many, many, {"batch": 1 - c}, 1).wait_send()


def finish(*refs):
    sources, results, sems = refs[:4], refs[4:8], refs[8]
    copies = [
        pltpu.make_async_copy(src, dst, sems.at[i])
        for i, (src, dst) in enumerate(zip(sources, results))
    ]
    for copy in copies:
        copy.start()
    for copy in copies:
        copy.wait()


GROUPS = 3 + 6 + 4 * 3 + 1 + 1 + 4 + 4 + 1 + 4
SENT = (
    3 * 64 + 6 * 256 + 18 * 80 + 26 * 256 + 4 * 320 + 3 * 320
    + 12 * 96 + 12 * 64 + 3 * 96 + 3 * 64 + 3 * 40
)


def body(inputs, cotangent, w_query, w_key, w_value):
    vmem = pltpu.VMEM
    hbm = pl.BlockSpec(memory_space=pl.ANY)
    scan = [
        vmem((4, 80, 128), f32), vmem((4, 80, 128), f32), vmem((80, 128), f32),
        vmem((3, 80, 128), f32), vmem((4, 80, 128), f32), vmem((4, 80, 128), f32),
    ]
    scratch = [
        vmem((BLK, D), bf16), vmem((BLK, 1024), bf16), vmem((D, 128), bf16), vmem((D, 128), bf16),
        vmem((4, D, 256), bf16), vmem((2, 4, 256, 128), f32), vmem((4, 8, 256, 128), f32),
        vmem((4, 64, 128), f32), vmem((3, 128, 256), f32), vmem((4, 64, 128), f32),
        vmem((4, 128, 256), f32), vmem((4, 128, 256), f32), vmem((4, 128, 256), f32),
        vmem((2, FP, TOK), bf16), vmem((2, FP, TOK), bf16), vmem((2, TOK, 128), bf16),
        vmem((2, 128, TOK), bf16), vmem((2, 128, TOK), f32), vmem((2, TOK, TOK), bf16),
        vmem((2, 128, TOK), f32), vmem((2, 8, TOK), f32), vmem((2, 128, TOK), bf16),
        vmem((2, 8, TOK), f32), vmem((2, FP, TOK), f32), vmem((2, FP, TOK), f32),
        vmem((2, 128, TOK), f32), vmem((2, FP, 128), bf16), vmem((2, 8, FP), f32),
        *scan, *scan,
        vmem((2, 4, 320, 128), f32), vmem((4, 320, 128), f32),
        vmem((D, BLK), f32), vmem((4, 4, 96, 128), f32), vmem((4, 4, 64, 128), f32),
        vmem((4, 3, 96, 128), f32), vmem((2, 4, 64, 128), f32),
        vmem((4, 96, 128), f32), vmem((3, 96, 128), f32), vmem((3, 64, 128), f32),
        vmem((4, 64, 128), f32),
        vmem((4, 40, 128), f32), vmem((4, 40, 128), f32),
        vmem((4, 40, 128), f32), vmem((SENT, 128), f32),
        pltpu.SemaphoreType.DMA((8,)), pltpu.SemaphoreType.DMA((2,)),
        pltpu.SemaphoreType.DMA((GROUPS,)),
    ]
    shapes = (((1, BLK, D), bf16), ((16, 128), f32), ((16, 128), f32), ((16, 1024), f32))
    results = pl.pallas_call(
        kernel,
        out_shape=tuple(pltpu.VMEM(*shape) for shape in shapes),
        in_specs=[pl.BlockSpec(memory_space=pltpu.HBM)] * 5,
        out_specs=(pl.BlockSpec(memory_space=pltpu.VMEM),) * 4,
        scratch_shapes=scratch,
        compiler_params=pltpu.CompilerParams(
            collective_id=0, has_side_effects=True, vmem_limit_bytes=60 * 1024 * 1024
        ),
    )(inputs, cotangent, w_query, w_key, w_value)
    return pl.pallas_call(
        finish,
        out_shape=tuple(jax.ShapeDtypeStruct(*shape) for shape in shapes),
        in_specs=[hbm] * 4,
        out_specs=(pl.BlockSpec(memory_space=pltpu.HBM),) * 4,
        scratch_shapes=[pltpu.SemaphoreType.DMA((4,))],
        compiler_params=pltpu.CompilerParams(vmem_limit_bytes=4 * 1024 * 1024),
    )(*results)


def solution(mesh):
    split = Mesh(
        mesh.devices.reshape(4, 4, 4, mesh.shape["batch"]), ("seq_0", "seq_1", "seq_2", "batch")
    )
    in_specs = (P("batch", SEQ, None), P("batch", SEQ, None), P(), P(), P())
    out_specs = (P("batch", SEQ, None), P(SEQ_BATCH, None), P(SEQ_BATCH, None), P(SEQ_BATCH, None))
    return jax.shard_map(body, mesh=split, in_specs=in_specs, out_specs=out_specs, check_vma=False)
```
